512 devices in a mesh: pix: 4 (over x_lo, core), scan: 128 (over x_hi, z, y).
Axes of the slice: x: 4 (x_hi: 2, x_lo: 2; x = x_hi * 2 + x_lo), y: 8, z: 8, core: 2. Of those that a mesh axis runs over, the one named last changes fastest.
Arguments:
- scan_data: bfloat16 [128, 512, 512], P('pix', 'scan'), may hold values from -6 to 6
- pixel_coords: int32 [2, 128], P(None, 'pix'), may hold values from -6 to 6, as said below
- aberrations: float32 [4], replicated, may hold values from -3 to 3
Outputs:
- object_wave: float32 [2, 512, 512], P(None, 'scan', 'pix')
The draws below stay inside these ranges and needn't reach their ends.
Inputs may be any that keep to these rules, and one draw needn't show every extreme that they name: `pixel_coords`: each column is a distinct pair (u, v) of integers with u * u + v * v <= 40; their order is arbitrary.
All inputs are finite; a program needn't handle non-finite values.
Results may differ from the reference program's by a relative error of at most 0.0043.
Values may be sent and summed in bfloat16 or wider, within the bound.
No kernel may reach another device: no remote copies, remote signals or barrier semaphores. Data moves between devices by JAX's collectives and lax.ppermute only.
A program may use at most 64 MiB of HBM per device.

```python
import math
import jax
import jax.numpy as jnp
from jax import lax

NX = 512
NY = 512
PIXELS = 128
STEP = 8


def draw_pixel_coords(key, part):
    lattice = jnp.arange(169, dtype=jnp.int32)
    along_u = lattice // 13 - 6
    along_v = lattice % 13 - 6
    inside = (along_u * along_u + along_v * along_v <= 40).astype(jnp.int32)
    shuffled = jax.random.permutation(key, 169).astype(jnp.int32)
    scores = inside * 1000 + shuffled
    ranking = jnp.argsort(-scores, stable=True)[:PIXELS]
    return jnp.stack([along_u[ranking], along_v[ranking]]).astype(jnp.int32)


def shard_levels(own_key, shape, shards, least, largest):
    loudness = 1.0
    for dim, parts in shards:
        heights = jax.random.uniform(jax.random.fold_in(jax.random.fold_in(own_key, 6), dim), (parts,), jnp.float32, least / len(shards), largest / len(shards))
        loudness = loudness * jnp.repeat(jnp.exp(heights), shape[dim] // parts).reshape((-1,) + (1,) * (len(shape) - 1 - dim))
    return loudness


def scatter_about(key, shape, width, most, cuts=(), held_as=jnp.bfloat16):
    result = width * jax.random.normal(key, shape, jnp.float32)
    if cuts:
        result = result * shard_levels(key, shape, cuts, -0.22, 0.18)
    return jnp.clip(result, -most, most).astype(held_as)


def setup_inputs(seed: int = 0) -> dict:
    keys = jax.random.split(jax.random.key(seed), 4)
    return {
        "scan_data": scatter_about(keys[0], (PIXELS, NX, NY), 1.0, 6.0, ((0, 4), (1, 128))),
        "pixel_coords": draw_pixel_coords(jax.random.fold_in(keys[3], 71), 0),
        "aberrations": jnp.clip(jax.random.uniform(keys[2], (4,), jnp.float32, -3.0, 3.0), -3.0, 3.0),
    }


full_turn = 2.0 * math.pi


def frequencies(length, banded):
    counter = jnp.arange(length // 2 if banded else length, dtype=jnp.int32)
    if banded:
        return jnp.where(counter < length // 4, counter, counter + length // 2).astype(jnp.int32)
    return counter


def signed_freq(spectral, length):
    return jnp.where(spectral < length // 2, spectral, spectral - length).astype(jnp.int32)


def phase_table(spectral, length, places):
    product = (spectral[:, None] * places[None, :]) % length
    angles = product.astype(jnp.float32) * (full_turn / length)
    return jnp.cos(angles), jnp.sin(angles)


def aberration(along_x, along_y, coefficients):
    aperture = 40.0 * STEP * STEP
    radial = (along_x * along_x + along_y * along_y) / aperture
    return (coefficients[0] * radial
            + coefficients[1] * (along_x * along_x - along_y * along_y) / aperture
            + coefficients[2] * 2.0 * along_x * along_y / aperture
            + coefficients[3] * radial * radial)


def trotter(column_u, column_v, freq_x, freq_y, coefficients):
    centre_x = STEP * column_u
    centre_y = STEP * column_v
    minus_x = centre_x - freq_x
    minus_y = centre_y - freq_y
    plus_x = centre_x + freq_x
    plus_y = centre_y + freq_y
    aperture_bound = 40 * STEP * STEP
    inside_minus = minus_x * minus_x + minus_y * minus_y <= aperture_bound
    inside_plus = plus_x * plus_x + plus_y * plus_y <= aperture_bound
    left_mask = jnp.logical_and(inside_minus, jnp.logical_not(inside_plus)).astype(jnp.float32)
    right_mask = jnp.logical_and(inside_plus, jnp.logical_not(inside_minus)).astype(jnp.float32)
    own_phase = aberration(centre_x.astype(jnp.float32), centre_y.astype(jnp.float32), coefficients)
    left_phase = aberration(minus_x.astype(jnp.float32), minus_y.astype(jnp.float32), coefficients) - own_phase
    right_phase = own_phase - aberration(plus_x.astype(jnp.float32), plus_y.astype(jnp.float32), coefficients)
    weight_real = left_mask * jnp.cos(left_phase) - right_mask * jnp.cos(right_phase)
    weight_imag = left_mask * jnp.sin(left_phase) - right_mask * jnp.sin(right_phase)
    return weight_real, weight_imag


def rounded(table):
    return lax.optimization_barrier(table.astype(jnp.bfloat16)).astype(jnp.float32)


def reference(scan_data, pixel_coords, aberrations):
    highest = lax.Precision.HIGHEST
    across = frequencies(NY, True)
    downward = frequencies(NX, True)
    cosine_rows, sine_rows = phase_table(jnp.arange(NY, dtype=jnp.int32), NY, across)
    cosine_rows = rounded(cosine_rows)
    sine_rows = rounded(sine_rows)
    inverse_cos_x, inverse_sin_x = phase_table(downward, NX, jnp.arange(NX, dtype=jnp.int32))
    cosine_cols = rounded(inverse_cos_x)
    sine_cols = rounded(inverse_sin_x)
    freq_x = signed_freq(downward, NX)[:, None]
    freq_y = signed_freq(across, NY)[None, :]

    def accumulate(totals, inputs):
        picture, coords = inputs
        picture = picture.astype(jnp.float32)
        real_rows = jnp.dot(picture, cosine_rows, precision=highest, preferred_element_type=jnp.float32).astype(jnp.bfloat16)
        imag_rows = (-jnp.dot(picture, sine_rows, precision=highest, preferred_element_type=jnp.float32)).astype(jnp.bfloat16)
        real_rows, imag_rows = lax.optimization_barrier((real_rows, imag_rows))
        real_rows = real_rows.astype(jnp.float32)
        imag_rows = imag_rows.astype(jnp.float32)
        spec_real = (jnp.dot(cosine_cols, real_rows, precision=highest, preferred_element_type=jnp.float32)
                     + jnp.dot(sine_cols, imag_rows, precision=highest, preferred_element_type=jnp.float32))
        spec_imag = (jnp.dot(cosine_cols, imag_rows, precision=highest, preferred_element_type=jnp.float32)
                     - jnp.dot(sine_cols, real_rows, precision=highest, preferred_element_type=jnp.float32))
        weight_real, weight_imag = trotter(coords[0], coords[1], freq_x, freq_y, aberrations)
        return (totals[0] + spec_real * weight_real - spec_imag * weight_imag,
                totals[1] + spec_real * weight_imag + spec_imag * weight_real), None

    initial = jnp.zeros((downward.shape[0], across.shape[0]), jnp.float32)
    (summed_real, summed_imag), _ = lax.scan(accumulate, (initial, initial), (scan_data, pixel_coords.T))
    column_real = (jnp.dot(inverse_cos_x.T, summed_real, precision=highest, preferred_element_type=jnp.float32)
                   - jnp.dot(inverse_sin_x.T, summed_imag, precision=highest, preferred_element_type=jnp.float32))
    column_imag = (jnp.dot(inverse_sin_x.T, summed_real, precision=highest, preferred_element_type=jnp.float32)
                   + jnp.dot(inverse_cos_x.T, summed_imag, precision=highest, preferred_element_type=jnp.float32))
    final_cos, final_sin = phase_table(across, NY, jnp.arange(NY, dtype=jnp.int32))
    object_real = (jnp.dot(column_real, final_cos, precision=highest, preferred_element_type=jnp.float32)
                   - jnp.dot(column_imag, final_sin, precision=highest, preferred_element_type=jnp.float32))
    object_imag = (jnp.dot(column_real, final_sin, precision=highest, preferred_element_type=jnp.float32)
                   + jnp.dot(column_imag, final_cos, precision=highest, preferred_element_type=jnp.float32))
    return jnp.stack([object_real, object_imag]) * (1.0 / (NX * NY))
```

```python
import functools
import math

import jax
import jax.numpy as jnp
import numpy as np
from jax import lax
from jax.experimental import pallas as pl
from jax.experimental.pallas import tpu as pltpu
from jax.sharding import Mesh, PartitionSpec as P

STEP = 8
N = 512
BAND = 256
BOUND = 40.0 * STEP * STEP
VMEM = pl.BlockSpec(memory_space=pltpu.VMEM)
SMEM = pl.BlockSpec(memory_space=pltpu.SMEM)
BF = jnp.bfloat16
F32 = jnp.float32


def angles(k, n):
    return 2.0 * math.pi * np.mod(k * n, N) / N


def split(table):
    hi = table.astype(np.float32).astype(BF)
    lo = (table - hi.astype(np.float64)).astype(np.float32).astype(BF)
    return hi, lo


@functools.lru_cache(None)
def tables():
    jj, yy, c = np.meshgrid(np.arange(4), np.arange(8), np.arange(4), indexing="ij")
    ky = (8 * (4 * c + jj) + yy)[..., None]
    t = angles(ky, np.arange(N))
    row = np.stack([np.cos(t), -np.sin(t)], axis=3).reshape(256, N).astype(np.float32).astype(BF)
    kx = np.arange(BAND) - BAND // 2
    t = angles(np.arange(N)[:, None], kx[None, :])
    cos, sin = np.cos(t), np.sin(t)
    col = np.stack([np.concatenate([cos, -sin], 1), np.concatenate([sin, cos], 1)], axis=1)
    col = col.reshape(16, 64, 2 * BAND).astype(np.float32).astype(BF)
    inv = split(np.concatenate([cos.T, sin.T], 1))
    yy, j = np.meshgrid(np.arange(8), np.arange(16), indexing="ij")
    ky = 8 * j + yy
    t = angles(ky[..., None], np.arange(N))
    fold = np.where(ky == 0, 1.0, 2.0)[..., None] / (N * N)
    real = np.where(ky == 0, 1.0, 0.0)[..., None] / (N * N)
    im = np.stack([np.sin(t) * fold, np.cos(t) * fold], axis=1)
    re = np.stack([np.cos(t) * real, -np.sin(t) * real], axis=1)
    fin = np.stack([re, im], axis=3).reshape(256, 2, 4, 128).transpose(2, 0, 1, 3).reshape(4, 256, 256)
    return row, col, inv, split(fin)


def swap_blocks(parts):
    lane = lax.broadcasted_iota(jnp.int32, parts[0].shape, 1) // 32
    out = []
    for m in range(4):
        acc = parts[0] if m == 0 else pltpu.roll(parts[0], (-32 * m) % 128, 1)
        for q in range(1, 4):
            shift = (32 * (q - m)) % 128
            moved = parts[q] if shift == 0 else pltpu.roll(parts[q], shift, 1)
            acc = jnp.where(lane == q, moved, acc)
        out.append(acc)
    return out


def row_kernel(table, data, out):
    spec = lax.dot_general(table[...], data[...], (((1,), (1,)), ((), ())), preferred_element_type=F32)
    moved = swap_blocks([spec[64 * q : 64 * q + 64] for q in range(4)])
    for r in range(4):
        out[:, r] = moved[r].reshape(8, 8, 128).astype(BF)


def weight_kernel(params, centres, w_re, w_im):
    a0 = params[0] / BOUND
    a1 = params[1] / BOUND
    a2 = params[2] * 2.0 / BOUND
    a3 = params[3] / (BOUND * BOUND)
    first = params[4]

    def chi(px, py, r2):
        return a0 * r2 + a1 * (px * px - py * py) + a2 * (px * py) + a3 * (r2 * r2)

    def one(j, carry):
        qy = first + 8.0 * j.astype(F32)
        rows = pl.ds(pl.multiple_of(j * 32, 32), 32)
        kx = centres[0]
        ky = centres[1]
        k2 = kx * kx + ky * ky
        own = chi(kx, ky, k2)
        for half in range(2):
            lanes = slice(128 * half, 128 * half + 128)
            qx = (lax.broadcasted_iota(jnp.int32, (32, 128), 1) + (128 * half - 128)).astype(F32)
            dot = 2.0 * (kx * qx + ky * qy)
            square = k2 + (qx * qx + qy * qy)
            near = square - jnp.abs(dot)
            far = square + jnp.abs(dot)
            sign = jnp.where(dot > 0.0, 1.0, -1.0)
            keep = jnp.where((near <= BOUND) & (far > BOUND), 1.0, 0.0)
            phase = chi(kx - sign * qx, ky - sign * qy, near) - own
            turns = jnp.floor(phase * (2.0 / math.pi) + 0.5)
            rest = phase - turns * 1.5703125
            rest = rest - turns * 4.837512969970703e-4
            rest = rest - turns * 7.549789954891882e-8
            z = rest * rest
            sine = rest + rest * z * (-1.0 / 6 + z * (1.0 / 120 + z * (-1.0 / 5040 + z * (1.0 / 362880))))
            cosine = 1.0 + z * (-0.5 + z * (1.0 / 24 + z * (-1.0 / 720 + z * (1.0 / 40320))))
            pair = jnp.floor(turns * 0.5)
            odd = turns - 2.0 * pair > 0.5
            flip = keep * (1.0 - 2.0 * (pair - 2.0 * jnp.floor(pair * 0.5)))
            w_re[rows, lanes] = flip * sign * jnp.where(odd, -sine, cosine)
            w_im[rows, lanes] = flip * jnp.where(odd, cosine, sine)
        return carry

    lax.fori_loop(0, 16, one, 0)


def column_kernel(rows, table, w_re, w_im, inv_hi, inv_lo, out, spec, total):
    held = rows[...].astype(F32).reshape(256, 128).T
    group = (lax.broadcasted_iota(jnp.int32, held.shape, 1) // 2) % 4
    stacked = jnp.concatenate([jnp.where(group == c, held, 0.0) for c in range(4)], axis=0).astype(BF)
    spec[...] = jnp.dot(stacked, table[...], preferred_element_type=F32)
    for j in range(16):
        part = slice(32 * j, 32 * j + 32)
        s_re, s_im = spec[part, :BAND], spec[part, BAND:]
        a, b = w_re[part, :], w_im[part, :]
        total[j : j + 1, :] = jnp.sum(s_re * a - s_im * b, axis=0, keepdims=True)
        total[16 + j : 17 + j, :] = jnp.sum(s_re * b + s_im * a, axis=0, keepdims=True)
    whole = total[...]
    hi = whole.astype(BF)
    lo = (whole - hi.astype(F32)).astype(BF)
    both = jnp.dot(jnp.concatenate([hi, lo], axis=0), inv_hi[...], preferred_element_type=F32)
    prod = both[:32] + both[32:] + jnp.dot(hi, inv_lo[...], preferred_element_type=F32)
    c_re = prod[:16, :N] - prod[16:, N:]
    c_im = prod[:16, N:] + prod[16:, :N]
    quarters = [c_re[:8], c_re[8:], c_im[:8], c_im[8:]]
    for t in range(4):
        moved = swap_blocks([v[:, 128 * t : 128 * t + 128] for v in quarters])
        for m in range(4):
            out[4 * t + m] = moved[m]


def regroup_kernel(params, parts, out):
    total = jnp.sum(parts[...], axis=0)
    rows = [total if q == 0 else pltpu.roll(total, 128 - 32 * q, 1) for q in range(4)]
    block = jnp.concatenate(rows * 4, axis=0)
    place = lax.broadcasted_iota(jnp.int32, block.shape, 0) // 32
    block = jnp.where(place == params[0] % 4, block, 0.0)
    turned = block.T
    for y in range(8):
        for g in range(4):
            out[8 * g + y] = turned[4 * y : 4 * y + 4]


def final_kernel(parts, hi_table, lo_table, out):
    halves = []
    for h in range(2):
        acc = None
        for g in range(4):
            piece = jnp.sum(parts[8 * g + 4 * h : 8 * g + 4 * h + 4], axis=0)
            acc = piece if acc is None else acc + piece
        halves.append(acc)
    whole = jnp.concatenate(halves, axis=1)
    hi = whole.astype(BF)
    lo = (whole - hi.astype(F32)).astype(BF)
    obj = jnp.dot(hi, hi_table[...], preferred_element_type=F32)
    obj = obj + jnp.dot(lo, hi_table[...], preferred_element_type=F32)
    obj = obj + jnp.dot(hi, lo_table[...], preferred_element_type=F32)
    out[0] = obj[:, :128]
    out[1] = obj[:, 128:]


def call(kernel, shapes, n_in, smem=0, scratch=()):
    single = not isinstance(shapes, (list, tuple))
    count = 1 if single else len(shapes)
    return pl.pallas_call(
        kernel,
        out_shape=shapes,
        in_specs=[SMEM] * smem + [VMEM] * (n_in - smem),
        out_specs=VMEM if single else [VMEM] * count,
        scratch_shapes=list(scratch),
    )


def on_device(scan_data, pixel_coords, aberrations):
    shape = jax.ShapeDtypeStruct
    row, col, (inv_hi, inv_lo), (fin_hi, fin_lo) = tables()
    y = lax.axis_index("y")
    block = lax.axis_index(("xh", "z"))
    group = lax.axis_index(("xl", "core"))

    data = scan_data.transpose(1, 0, 2).reshape(128, N)
    rows = call(row_kernel, shape((8, 4, 8, 128), BF), 2)(jnp.asarray(row), data)
    rows = lax.all_to_all(rows, "y", 0, 0, tiled=True)

    params = jnp.concatenate([aberrations, y.astype(F32)[None]])
    centres = jnp.broadcast_to((STEP * pixel_coords).astype(F32)[:, :, None], (2, 32, 128))
    w_re, w_im = call(weight_kernel, [shape((512, BAND), F32)] * 2, 2, smem=1)(params, centres)
    table = lax.dynamic_index_in_dim(jnp.asarray(col), block, 0, keepdims=False)
    table = jnp.broadcast_to(table.reshape(32, 1, 2, N), (32, 4, 2, N)).reshape(256, N)

    partial = call(
        column_kernel,
        shape((16, 8, 128), F32),
        6,
        scratch=[pltpu.VMEM((512, N), F32), pltpu.VMEM((32, BAND), F32)],
    )(rows, table, w_re, w_im, jnp.asarray(inv_hi), jnp.asarray(inv_lo))
    partial = lax.all_to_all(partial, ("xh", "z"), 0, 0, tiled=True)
    pieces = call(regroup_kernel, shape((32, 4, 128), F32), 2, smem=1)(y[None], partial)
    pieces = lax.all_to_all(pieces, ("xl", "core", "y"), 0, 0, tiled=True)
    hi = lax.dynamic_index_in_dim(jnp.asarray(fin_hi), group, 0, keepdims=False)
    lo = lax.dynamic_index_in_dim(jnp.asarray(fin_lo), group, 0, keepdims=False)
    return call(final_kernel, shape((2, 4, 128), F32), 3)(pieces, hi, lo)


def solution(mesh):
    axes = ("xl", "core", "xh", "z", "y")
    fine = Mesh(mesh.devices.reshape(2, 2, 2, 8, 8), axes)
    pix, scan = ("xl", "core"), ("xh", "z", "y")
    placed = (P(pix, scan, None), P(None, pix), P())
    return jax.shard_map(
        on_device, mesh=fine, in_specs=placed, out_specs=P(None, scan, pix), check_vma=False
    )
```

```python
import functools
import math

import jax
import jax.numpy as jnp
import numpy as np
from jax import lax
from jax.experimental import pallas as pl
from jax.experimental.pallas import tpu as pltpu
from jax.sharding import Mesh, PartitionSpec as P

STEP = 8
N = 512
BAND = 256
BOUND = 40.0 * STEP * STEP
VMEM = pl.BlockSpec(memory_space=pltpu.VMEM)
KEPT = pl.BlockSpec(memory_space=pltpu.VMEM)
SMEM = pl.BlockSpec(memory_space=pltpu.SMEM)
ANY = pl.BlockSpec(memory_space=pltpu.HBM)
BF = jnp.bfloat16
F32 = jnp.float32


def angles(k, n):
    return 2.0 * math.pi * np.mod(k * n, N) / N


def split(table):
    hi = table.astype(np.float32).astype(BF)
    lo = (table - hi.astype(np.float64)).astype(np.float32).astype(BF)
    return hi, lo


@functools.lru_cache(None)
def tables():
    jj, yy, c = np.meshgrid(np.arange(4), np.arange(8), np.arange(4), indexing="ij")
    ky = (8 * (4 * c + jj) + yy)[..., None]
    t = angles(ky, np.arange(N))
    row = np.stack([np.cos(t), -np.sin(t)], axis=3).reshape(256, N).astype(np.float32).astype(BF)
    kx = np.arange(BAND) - BAND // 2
    t = angles(np.arange(N)[:, None], kx[None, :])
    cos, sin = np.cos(t), np.sin(t)
    col = np.stack([np.concatenate([cos, -sin], 1), np.concatenate([sin, cos], 1)], axis=1)
    col = col.reshape(16, 64, 2 * BAND).astype(np.float32).astype(BF)
    inv = split(np.concatenate([cos.T, sin.T], 1))
    yy, j = np.meshgrid(np.arange(8), np.arange(16), indexing="ij")
    ky = 8 * j + yy
    t = angles(ky[..., None], np.arange(N))
    fold = np.where(ky == 0, 1.0, 2.0)[..., None] / (N * N)
    real = np.where(ky == 0, 1.0, 0.0)[..., None] / (N * N)
    im = np.stack([np.sin(t) * fold, np.cos(t) * fold], axis=1)
    re = np.stack([np.cos(t) * real, -np.sin(t) * real], axis=1)
    fin = np.stack([re, im], axis=3).reshape(256, 2, 4, 128).transpose(2, 0, 1, 3).reshape(4, 256, 256)
    repeat = np.zeros((256, 64), np.float32)
    lane = np.arange(256)
    repeat[lane, lane // 8 * 2 + lane % 2] = 1.0
    fin = np.stack(split(fin), axis=1)
    return row, repeat.astype(BF), col, np.stack(inv), fin


def swap_blocks(parts):
    lane = lax.broadcasted_iota(jnp.int32, parts[0].shape, 1) // 32
    out = []
    for m in range(4):
        acc = parts[0] if m == 0 else pltpu.roll(parts[0], (-32 * m) % 128, 1)
        for q in range(1, 4):
            shift = (32 * (q - m)) % 128
            moved = parts[q] if shift == 0 else pltpu.roll(parts[q], shift, 1)
            acc = jnp.where(lane == q, moved, acc)
        out.append(acc)
    return out


def row_kernel(table, data, out):
    held = data[...].reshape(128, N)
    spec = lax.dot_general(table[...], held, (((1,), (1,)), ((), ())), preferred_element_type=F32)
    source = lax.broadcasted_iota(jnp.int32, (128, 128), 0)
    target = lax.broadcasted_iota(jnp.int32, (128, 128), 1)
    order = jnp.where(source == (target % 32) * 4 + target // 32, 1.0, 0.0).astype(BF)
    spec = jnp.dot(spec.astype(BF), order, preferred_element_type=F32)
    moved = swap_blocks([spec[64 * q : 64 * q + 64] for q in range(4)])
    for r in range(4):
        out[:, r] = moved[r].reshape(8, 8, 128).astype(BF)


def weight_kernel(coefficients, coords, repeat, col, inv, fin, w_re, w_im, table, inv_out, fin_out, block, sems):
    here = lax.axis_index("xh") * 8 + lax.axis_index("z")
    group = lax.axis_index("xl") * 2 + lax.axis_index("core")
    copies = [
        pltpu.make_async_copy(col.at[here], block, sems.at[0]),
        pltpu.make_async_copy(inv, inv_out, sems.at[1]),
        pltpu.make_async_copy(fin.at[group], fin_out, sems.at[2]),
    ]
    for copy in copies:
        copy.start()

    a0 = coefficients[0] / BOUND
    a1 = coefficients[1] / BOUND
    a2 = coefficients[2] * 2.0 / BOUND
    a3 = coefficients[3] / (BOUND * BOUND)
    first = lax.axis_index("y").astype(F32)

    def chi(px, py, r2):
        return a0 * r2 + a1 * (px * px - py * py) + a2 * (px * py) + a3 * (r2 * r2)

    centre = coords[...].astype(F32) * float(STEP)
    kx = jnp.broadcast_to(centre[0:1], (128, 32)).T
    ky = jnp.broadcast_to(centre[1:2], (128, 32)).T
    k2 = kx * kx + ky * ky
    own = chi(kx, ky, k2)

    def one(j, carry):
        qy = first + 8.0 * j.astype(F32)
        rows = pl.ds(pl.multiple_of(j * 32, 32), 32)
        for half in range(2):
            lanes = slice(128 * half, 128 * half + 128)
            qx = (lax.broadcasted_iota(jnp.int32, (32, 128), 1) + (128 * half - 128)).astype(F32)
            dot = 2.0 * (kx * qx + ky * qy)
            square = k2 + (qx * qx + qy * qy)
            near = square - jnp.abs(dot)
            far = square + jnp.abs(dot)
            sign = jnp.where(dot > 0.0, 1.0, -1.0)
            keep = jnp.where((near <= BOUND) & (far > BOUND), 1.0, 0.0)
            phase = chi(kx - sign * qx, ky - sign * qy, near) - own
            turns = jnp.floor(phase * (2.0 / math.pi) + 0.5)
            rest = phase - turns * 1.5703125
            rest = rest - turns * 4.837512969970703e-4
            rest = rest - turns * 7.549789954891882e-8
            z = rest * rest
            sine = rest + rest * z * (-1.0 / 6 + z * (1.0 / 120 + z * (-1.0 / 5040 + z * (1.0 / 362880))))
            cosine = 1.0 + z * (-0.5 + z * (1.0 / 24 + z * (-1.0 / 720 + z * (1.0 / 40320))))
            pair = jnp.floor(turns * 0.5)
            odd = turns - 2.0 * pair > 0.5
            flip = keep * (1.0 - 2.0 * (pair - 2.0 * jnp.floor(pair * 0.5)))
            w_re[rows, lanes] = flip * sign * jnp.where(odd, -sine, cosine)
            w_im[rows, lanes] = flip * jnp.where(odd, cosine, sine)
        return carry

    lax.fori_loop(0, 16, one, 0)
    copies[0].wait()
    table[...] = jnp.dot(repeat[...], block[...], preferred_element_type=F32).astype(BF)
    copies[1].wait()
    copies[2].wait()


def column_kernel(rows, table, w_re, w_im, inv, out, spec, total):
    held = rows[...].astype(F32).reshape(256, 128).T
    group = (lax.broadcasted_iota(jnp.int32, held.shape, 1) // 2) % 4
    stacked = jnp.concatenate([jnp.where(group == c, held, 0.0) for c in range(4)], axis=0).astype(BF)
    spec[...] = jnp.dot(stacked, table[...], preferred_element_type=F32)
    for j in range(16):
        part = slice(32 * j, 32 * j + 32)
        s_re, s_im = spec[part, :BAND], spec[part, BAND:]
        a, b = w_re[part, :], w_im[part, :]
        total[j : j + 1, :] = jnp.sum(s_re * a - s_im * b, axis=0, keepdims=True)
        total[16 + j : 17 + j, :] = jnp.sum(s_re * b + s_im * a, axis=0, keepdims=True)
    whole = total[...]
    hi = whole.astype(BF)
    lo = (whole - hi.astype(F32)).astype(BF)
    both = jnp.dot(jnp.concatenate([hi, lo], axis=0), inv[0], preferred_element_type=F32)
    prod = both[:32] + both[32:] + jnp.dot(hi, inv[1], preferred_element_type=F32)
    c_re = prod[:16, :N] - prod[16:, N:]
    c_im = prod[:16, N:] + prod[16:, :N]
    quarters = [c_re[:8], c_re[8:], c_im[:8], c_im[8:]]
    for t in range(4):
        moved = swap_blocks([v[:, 128 * t : 128 * t + 128] for v in quarters])
        for m in range(4):
            out[4 * t + m] = moved[m]


def regroup_kernel(parts, out):
    total = jnp.sum(parts[...], axis=0)
    rows = [total if q == 0 else pltpu.roll(total, 128 - 32 * q, 1) for q in range(4)]
    block = jnp.concatenate(rows * 4, axis=0)
    place = lax.broadcasted_iota(jnp.int32, block.shape, 0) // 32
    block = jnp.where(place == lax.axis_index("y") % 4, block, 0.0)
    turned = block.T
    for y in range(8):
        for g in range(4):
            out[8 * g + y] = turned[4 * y : 4 * y + 4]


def final_kernel(parts, table, out):
    halves = []
    for h in range(2):
        acc = None
        for g in range(4):
            piece = jnp.sum(parts[8 * g + 4 * h : 8 * g + 4 * h + 4], axis=0)
            acc = piece if acc is None else acc + piece
        halves.append(acc)
    whole = jnp.concatenate(halves, axis=1)
    hi = whole.astype(BF)
    lo = (whole - hi.astype(F32)).astype(BF)
    obj = jnp.dot(hi, table[0], preferred_element_type=F32)
    obj = obj + jnp.dot(lo, table[0], preferred_element_type=F32)
    obj = obj + jnp.dot(hi, table[1], preferred_element_type=F32)
    out[0] = obj[:, :128]
    out[1] = obj[:, 128:]


def call(kernel, shapes, specs, operands, scratch=()):
    single = not isinstance(shapes, (list, tuple))
    count = 1 if single else len(shapes)
    place = [pltpu.VMEM if spec is KEPT else pltpu.HBM for spec in specs]
    held = [pltpu.with_memory_space_constraint(x, space) for x, space in zip(operands, place)]
    return pl.pallas_call(
        kernel,
        out_shape=shapes,
        in_specs=specs,
        out_specs=VMEM if single else [VMEM] * count,
        scratch_shapes=list(scratch),
        compiler_params=pltpu.CompilerParams(vmem_limit_bytes=16 * 2**20),
    )(*held)


def on_device(scan_data, pixel_coords, aberrations):
    row, repeat, col, inv, fin = (jnp.asarray(t) for t in tables())
    shape = pltpu.VMEM
    rows = call(row_kernel, shape((8, 4, 8, 128), BF), [VMEM] * 2, (row, scan_data))
    rows = lax.all_to_all(rows, "y", 0, 0, tiled=True)
    w_re, w_im, table, inv, fin = call(
        weight_kernel,
        [
            shape((512, BAND), F32),
            shape((512, BAND), F32),
            shape((256, N), BF),
            shape((2, 256, 2 * N), BF),
            shape((2, 256, 256), BF),
        ],
        [SMEM, VMEM, VMEM, ANY, ANY, ANY],
        (aberrations, pixel_coords, repeat, col, inv, fin),
        scratch=[pltpu.VMEM((64, N), BF), pltpu.SemaphoreType.DMA((3,))],
    )
    partial = call(
        column_kernel,
        shape((16, 8, 128), F32),
        [KEPT] * 5,
        (rows, table, w_re, w_im, inv),
        scratch=[pltpu.VMEM((512, N), F32), pltpu.VMEM((32, BAND), F32)],
    )
    partial = lax.all_to_all(partial, ("xh", "z"), 0, 0, tiled=True)
    pieces = call(regroup_kernel, shape((32, 4, 128), F32), [KEPT], (partial,))
    pieces = lax.all_to_all(pieces, ("xl", "core", "y"), 0, 0, tiled=True)
    return call(final_kernel, jax.ShapeDtypeStruct((2, 4, 128), F32), [KEPT] * 2, (pieces, fin))


def solution(mesh):
    axes = ("xl", "core", "xh", "z", "y")
    fine = Mesh(mesh.devices.reshape(2, 2, 2, 8, 8), axes)
    pix, scan = ("xl", "core"), ("xh", "z", "y")
    placed = (P(pix, scan, None), P(None, pix), P())
    return jax.shard_map(
        on_device, mesh=fine, in_specs=placed, out_specs=P(None, scan, pix), check_vma=False
    )
```

```python
import functools
import math

import jax
import jax.numpy as jnp
import numpy as np
from jax import lax
from jax.experimental import pallas as pl
from jax.experimental.pallas import tpu as pltpu
from jax.sharding import Mesh, PartitionSpec as P

STEP = 8
N = 512
BAND = 256
BOUND = 40.0 * STEP * STEP
VMEM = pl.BlockSpec(memory_space=pltpu.VMEM)
KEPT = pl.BlockSpec(memory_space=pltpu.VMEM)
SMEM = pl.BlockSpec(memory_space=pltpu.SMEM)
ANY = pl.BlockSpec(memory_space=pltpu.HBM)
BF = jnp.bfloat16
F32 = jnp.float32


def angles(k, n):
    return 2.0 * math.pi * np.mod(k * n, N) / N


def split(table):
    hi = table.astype(np.float32).astype(BF)
    lo = (table - hi.astype(np.float64)).astype(np.float32).astype(BF)
    return hi, lo


@functools.lru_cache(None)
def tables():
    jj, yy, c = np.meshgrid(np.arange(4), np.arange(8), np.arange(4), indexing="ij")
    ky = (8 * (4 * c + jj) + yy)[..., None]
    t = angles(ky, np.arange(N))
    row = np.stack([np.cos(t), -np.sin(t)], axis=3).reshape(256, N).astype(np.float32).astype(BF)
    kx = np.arange(BAND) - BAND // 2
    t = angles(np.arange(N)[:, None], kx[None, :])
    cos, sin = np.cos(t), np.sin(t)
    col = np.stack([np.concatenate([cos, -sin], 1), np.concatenate([sin, cos], 1)], axis=1)
    col = col.reshape(16, 64, 2 * BAND).astype(np.float32).astype(BF)
    place = (np.arange(16)[:, None, None] * 32 + np.arange(4)[:, None] + 4 * np.arange(8)).reshape(-1)
    inv = split(np.concatenate([cos.T[:, place], sin.T[:, place]], 1))
    yy, j = np.meshgrid(np.arange(8), np.arange(16), indexing="ij")
    ky = 8 * j + yy
    t = angles(ky[..., None], np.arange(N))
    fold = np.where(ky == 0, 1.0, 2.0)[..., None] / (N * N)
    real = np.where(ky == 0, 1.0, 0.0)[..., None] / (N * N)
    im = np.stack([np.sin(t) * fold, np.cos(t) * fold], axis=1)
    re = np.stack([np.cos(t) * real, -np.sin(t) * real], axis=1)
    fin = np.stack([re, im], axis=3).reshape(256, 2, 4, 128).transpose(2, 0, 1, 3).reshape(4, 256, 256)
    fin = np.stack(split(fin), axis=1)
    return row, col, np.stack(inv), fin


def swap_blocks(parts):
    lane = lax.broadcasted_iota(jnp.int32, parts[0].shape, 1) // 32
    out = []
    for m in range(4):
        acc = parts[0] if m == 0 else pltpu.roll(parts[0], (-32 * m) % 128, 1)
        for q in range(1, 4):
            shift = (32 * (q - m)) % 128
            moved = parts[q] if shift == 0 else pltpu.roll(parts[q], shift, 1)
            acc = jnp.where(lane == q, moved, acc)
        out.append(acc)
    return out


def row_kernel(table, data, out):
    held = data[...].reshape(128, N)
    spec = lax.dot_general(table[...], held, (((1,), (1,)), ((), ())), preferred_element_type=F32)
    source = lax.broadcasted_iota(jnp.int32, (128, 128), 0)
    target = lax.broadcasted_iota(jnp.int32, (128, 128), 1)
    order = jnp.where(source == (target % 32) * 4 + target // 32, 1.0, 0.0).astype(BF)
    spec = jnp.dot(spec.astype(BF), order, preferred_element_type=F32)
    moved = swap_blocks([spec[64 * q : 64 * q + 64] for q in range(4)])
    for r in range(4):
        out[:, r] = moved[r].reshape(8, 8, 128).astype(BF)


def weight_kernel(coefficients, coords, col, inv, fin, w_re, w_im, table, inv_out, fin_out, block, sems):
    here = lax.axis_index("xh") * 8 + lax.axis_index("z")
    group = lax.axis_index("xl") * 2 + lax.axis_index("core")
    copies = [
        pltpu.make_async_copy(col.at[here], block, sems.at[0]),
        pltpu.make_async_copy(inv, inv_out, sems.at[1]),
        pltpu.make_async_copy(fin.at[group], fin_out, sems.at[2]),
    ]
    for copy in copies:
        copy.start()

    a0 = coefficients[0] / BOUND
    a1 = coefficients[1] / BOUND
    a2 = coefficients[2] * 2.0 / BOUND
    a3 = coefficients[3] / (BOUND * BOUND)
    first = lax.axis_index("y").astype(F32)

    def chi(px, py, r2):
        return a0 * r2 + a1 * (px * px - py * py) + a2 * (px * py) + a3 * (r2 * r2)

    centre = coords[...].astype(F32) * float(STEP)
    kx = jnp.broadcast_to(centre[0:1], (128, 32)).T
    ky = jnp.broadcast_to(centre[1:2], (128, 32)).T
    k2 = kx * kx + ky * ky
    own = chi(kx, ky, k2)

    def one(j, carry):
        qy = first + 8.0 * j.astype(F32)
        rows = pl.ds(pl.multiple_of(j * 32, 32), 32)
        for half in range(2):
            lanes = slice(128 * half, 128 * half + 128)
            qx = (lax.broadcasted_iota(jnp.int32, (32, 128), 1) + (128 * half - 128)).astype(F32)
            dot = 2.0 * (kx * qx + ky * qy)
            square = k2 + (qx * qx + qy * qy)
            near = square - jnp.abs(dot)
            far = square + jnp.abs(dot)
            sign = jnp.where(dot > 0.0, 1.0, -1.0)
            keep = jnp.where((near <= BOUND) & (far > BOUND), 1.0, 0.0)
            phase = chi(kx - sign * qx, ky - sign * qy, near) - own
            turns = jnp.floor(phase * (2.0 / math.pi) + 0.5)
            rest = phase - turns * 1.5703125
            rest = rest - turns * 4.837512969970703e-4
            rest = rest - turns * 7.549789954891882e-8
            z = rest * rest
            sine = rest + rest * z * (-1.0 / 6 + z * (1.0 / 120 + z * (-1.0 / 5040 + z * (1.0 / 362880))))
            cosine = 1.0 + z * (-0.5 + z * (1.0 / 24 + z * (-1.0 / 720 + z * (1.0 / 40320))))
            pair = jnp.floor(turns * 0.5)
            odd = turns - 2.0 * pair > 0.5
            flip = keep * (1.0 - 2.0 * (pair - 2.0 * jnp.floor(pair * 0.5)))
            w_re[rows, lanes] = flip * sign * jnp.where(odd, -sine, cosine)
            w_im[rows, lanes] = flip * jnp.where(odd, cosine, sine)
        return carry

    lax.fori_loop(0, 16, one, 0)
    copies[0].wait()
    target = lax.broadcasted_iota(jnp.int32, (256, 64), 0)
    source = lax.broadcasted_iota(jnp.int32, (256, 64), 1)
    repeat = jnp.where(source == target // 8 * 2 + target % 2, 1.0, 0.0).astype(BF)
    table[...] = jnp.dot(repeat, block[...], preferred_element_type=F32).astype(BF)
    copies[1].wait()
    copies[2].wait()


def column_kernel(rows, table, w_re, w_im, inv, out, spec, total):
    held = rows[...].astype(F32).reshape(256, 128).T
    group = (lax.broadcasted_iota(jnp.int32, held.shape, 1) // 2) % 4
    stacked = jnp.concatenate([jnp.where(group == c, held, 0.0) for c in range(4)], axis=0).astype(BF)
    spec[...] = jnp.dot(stacked, table[...], preferred_element_type=F32)
    for j in range(16):
        part = slice(32 * j, 32 * j + 32)
        s_re, s_im = spec[part, :BAND], spec[part, BAND:]
        a, b = w_re[part, :], w_im[part, :]
        total[j : j + 1, :] = jnp.sum(s_re * a - s_im * b, axis=0, keepdims=True)
        total[16 + j : 17 + j, :] = jnp.sum(s_re * b + s_im * a, axis=0, keepdims=True)
    whole = total[...]
    hi = whole.astype(BF)
    lo = (whole - hi.astype(F32)).astype(BF)
    both = jnp.dot(jnp.concatenate([hi, lo], axis=0), inv[0], preferred_element_type=F32)
    prod = both[:32] + both[32:] + jnp.dot(hi, inv[1], preferred_element_type=F32)
    c_re = prod[:16, :N] - prod[16:, N:]
    c_im = prod[:16, N:] + prod[16:, :N]
    quarters = [c_re[:8], c_re[8:], c_im[:8], c_im[8:]]
    for t in range(4):
        moved = swap_blocks([v[:, 128 * t : 128 * t + 128] for v in quarters])
        for m in range(4):
            out[4 * (t % 2) + m, t // 2] = moved[m]


def regroup_kernel(parts, out):
    blocks = []
    for half in range(2):
        total = jnp.sum(parts[:, half], axis=0)
        blocks += [total if q == 0 else pltpu.roll(total, 128 - 32 * q, 1) for q in range(4)]
    turned = jnp.concatenate(blocks * 2, axis=0).T
    lane = lax.broadcasted_iota(jnp.int32, (8, 128), 1) // 32
    for half in range(2):
        acc = jnp.zeros((8, 128), F32)
        for r in range(4):
            piece = turned[8 * r : 8 * r + 8]
            shift = 32 * (r - half) % 128
            acc = jnp.where(lane == r, piece if shift == 0 else pltpu.roll(piece, shift, 1), acc)
        for g in range(4):
            out[16 * g + 8 * half : 16 * g + 8 * half + 8] = acc


def final_kernel(parts, table, out):
    total = parts[0:8]
    for n in range(1, 8):
        total = total + parts[8 * n : 8 * n + 8]
    turns = [total if s == 0 else pltpu.roll(total, 32 * s, 1) for s in range(4)]
    row = lax.broadcasted_iota(jnp.int32, (8, 128), 0) % 4
    lane = lax.broadcasted_iota(jnp.int32, (8, 128), 1) // 32
    rows = []
    for r in range(4):
        spread = jnp.zeros((8, 128), F32)
        for a in range(4):
            spread = jnp.where((row == a) & (lane == a), turns[(a - r) % 4], spread)
        low = jnp.sum(spread[:4], axis=0, keepdims=True)
        high = jnp.sum(spread[4:], axis=0, keepdims=True)
        rows.append(jnp.concatenate([low, high], axis=1))
    whole = jnp.concatenate(rows, axis=0)
    hi = whole.astype(BF)
    lo = (whole - hi.astype(F32)).astype(BF)
    both = jnp.dot(jnp.concatenate([hi, lo], axis=0), table[0], preferred_element_type=F32)
    obj = both[:4] + both[4:] + jnp.dot(hi, table[1], preferred_element_type=F32)
    out[0] = obj[:, :128]
    out[1] = obj[:, 128:]


def call(kernel, shapes, specs, operands, scratch=()):
    single = not isinstance(shapes, (list, tuple))
    count = 1 if single else len(shapes)
    place = [pltpu.VMEM if spec is KEPT else pltpu.HBM for spec in specs]
    held = [pltpu.with_memory_space_constraint(x, space) for x, space in zip(operands, place)]
    return pl.pallas_call(
        kernel,
        out_shape=shapes,
        in_specs=specs,
        out_specs=VMEM if single else [VMEM] * count,
        scratch_shapes=list(scratch),
        compiler_params=pltpu.CompilerParams(vmem_limit_bytes=16 * 2**20),
    )(*held)


def on_device(scan_data, pixel_coords, aberrations):
    row, col, inv, fin = (jnp.asarray(t) for t in tables())
    shape = pltpu.VMEM
    rows = call(row_kernel, shape((8, 4, 8, 128), BF), [VMEM] * 2, (row, scan_data))
    rows = lax.all_to_all(rows, "y", 0, 0, tiled=True)
    w_re, w_im, table, inv, fin = call(
        weight_kernel,
        [
            shape((512, BAND), F32),
            shape((512, BAND), F32),
            shape((256, N), BF),
            shape((2, 256, 2 * N), BF),
            shape((2, 256, 256), BF),
        ],
        [SMEM, VMEM, ANY, ANY, ANY],
        (aberrations, pixel_coords, col, inv, fin),
        scratch=[pltpu.VMEM((64, N), BF), pltpu.SemaphoreType.DMA((3,))],
    )
    partial = call(
        column_kernel,
        shape((8, 2, 8, 128), F32),
        [KEPT] * 5,
        (rows, table, w_re, w_im, inv),
        scratch=[pltpu.VMEM((512, N), F32), pltpu.VMEM((32, BAND), F32)],
    )
    partial = lax.all_to_all(partial, "z", 0, 0, tiled=True)
    pieces = call(regroup_kernel, shape((64, 128), F32), [KEPT], (partial,))
    pieces = lax.all_to_all(pieces.reshape(64, 1, 128), ("xl", "core", "xh", "y"), 0, 0, tiled=True)
    return call(final_kernel, jax.ShapeDtypeStruct((2, 4, 128), F32), [KEPT] * 2, (pieces.reshape(64, 128), fin))


def solution(mesh):
    axes = ("xl", "core", "xh", "z", "y")
    fine = Mesh(mesh.devices.reshape(2, 2, 2, 8, 8), axes)
    pix, scan = ("xl", "core"), ("xh", "z", "y")
    placed = (P(pix, scan, None), P(None, pix), P())
    return jax.shard_map(
        on_device, mesh=fine, in_specs=placed, out_specs=P(None, scan, pix), check_vma=False
    )
```

```python
import functools
import math

import jax
import jax.numpy as jnp
import numpy as np
from jax import lax
from jax.experimental import pallas as pl
from jax.experimental.pallas import tpu as pltpu
from jax.sharding import Mesh, PartitionSpec as P

STEP = 8
N = 512
BAND = 256
BOUND = 40.0 * STEP * STEP
LIVE = 26
VMEM = pl.BlockSpec(memory_space=pltpu.VMEM)
KEPT = pl.BlockSpec(memory_space=pltpu.VMEM)
SMEM = pl.BlockSpec(memory_space=pltpu.SMEM)
ANY = pl.BlockSpec(memory_space=pltpu.HBM)
BF = jnp.bfloat16
F32 = jnp.float32
WIRE = BF
PIX = ("xl", "core")
SCAN = ("xh", "zh", "zl", "yh", "yl")


def angles(k, n):
    return 2.0 * math.pi * np.mod(k * n, N) / N


def split(table):
    hi = table.astype(np.float32).astype(BF)
    lo = (table - hi.astype(np.float64)).astype(np.float32).astype(BF)
    return hi, lo


@functools.lru_cache(None)
def tables():
    jj, m, c = np.meshgrid(np.arange(4), np.arange(4), np.arange(8), indexing="ij")
    ky = (4 * (4 * c + jj) + m)[..., None]
    t = angles(ky, np.arange(N))
    row = np.stack([np.cos(t), -np.sin(t)], axis=3).reshape(256, N).astype(np.float32).astype(BF)
    kx = np.arange(BAND) - BAND // 2
    t = angles(np.arange(N)[:, None], kx[None, :])
    cos, sin = np.cos(t), np.sin(t)
    col = np.stack([np.concatenate([cos, -sin], 1), np.concatenate([sin, cos], 1)], axis=1)
    col = col.reshape(2, 4, 2, 4, 2, 4, 2, 2 * BAND).transpose(0, 1, 3, 2, 4, 5, 6, 7)
    col = col.reshape(32, 32, 2 * BAND).astype(np.float32).astype(BF)
    inv = split(np.concatenate([cos.T, sin.T], 1))
    yl, zl, j = np.meshgrid(np.arange(2), np.arange(2), np.arange(32), indexing="ij")
    ky = 4 * j + 2 * zl + yl
    t = angles(ky[..., None], np.arange(N))
    fold = np.where(ky == 0, 1.0, 2.0)[..., None] / (N * N)
    real = np.where(ky == 0, 1.0, 0.0)[..., None] / (N * N)
    im = np.stack([np.sin(t) * fold, np.cos(t) * fold], axis=2)
    re = np.stack([np.cos(t) * real, -np.sin(t) * real], axis=2)
    fin = np.stack([re, im], axis=4).reshape(256, 2, 4, 128).transpose(2, 0, 1, 3).reshape(4, 256, 256)
    fin = np.stack(split(fin), axis=1)
    return row, col, np.stack(inv), fin


def swap_blocks(parts):
    lane = lax.broadcasted_iota(jnp.int32, parts[0].shape, 1) // 32
    out = []
    for m in range(4):
        acc = parts[0] if m == 0 else pltpu.roll(parts[0], (-32 * m) % 128, 1)
        for q in range(1, 4):
            shift = (32 * (q - m)) % 128
            moved = parts[q] if shift == 0 else pltpu.roll(parts[q], shift, 1)
            acc = jnp.where(lane == q, moved, acc)
        out.append(acc)
    return out


def row_kernel(table, data, out):
    held = data[...].reshape(128, N)
    spec = lax.dot_general(table[...], held, (((1,), (1,)), ((), ())), preferred_element_type=F32)
    source = lax.broadcasted_iota(jnp.int32, (128, 128), 0)
    target = lax.broadcasted_iota(jnp.int32, (128, 128), 1)
    order = jnp.where(source == (target % 32) * 4 + target // 32, 1.0, 0.0).astype(BF)
    spec = jnp.dot(spec.astype(BF), order, preferred_element_type=F32)
    moved = swap_blocks([spec[64 * q : 64 * q + 64] for q in range(4)])
    for r in range(4):
        out[:, r] = moved[r].reshape(4, 16, 128).astype(BF)


def weight_kernel(coefficients, coords, col, inv, fin, w_re, w_im, table, inv_out, fin_out, block, sems):
    here = (lax.axis_index("xh") * 4 + lax.axis_index("zh")) * 4 + lax.axis_index("yh")
    group = lax.axis_index("xl") * 2 + lax.axis_index("core")
    copies = [
        pltpu.make_async_copy(col.at[here], block, sems.at[0]),
        pltpu.make_async_copy(inv, inv_out, sems.at[1]),
        pltpu.make_async_copy(fin.at[group], fin_out, sems.at[2]),
    ]
    for copy in copies:
        copy.start()

    a0 = coefficients[0] / (BOUND * math.pi)
    a1 = coefficients[1] / (BOUND * math.pi)
    a2 = coefficients[2] * 2.0 / (BOUND * math.pi)
    a3 = coefficients[3] / (BOUND * BOUND * math.pi)
    first = (2 * lax.axis_index("zl") + lax.axis_index("yl")).astype(F32)

    def chi(px, py, x2, y2, r2):
        return r2 * (a0 + a3 * r2) + (a1 * (x2 - y2) + a2 * (px * py))

    centre = coords[...].astype(F32) * float(STEP)
    kx = jnp.broadcast_to(centre[0:1], (128, 32)).T
    ky = jnp.broadcast_to(centre[1:2], (128, 32)).T
    own = chi(kx, ky, kx * kx, ky * ky, kx * kx + ky * ky)

    def one(j, carry):
        qy = first + 4.0 * j.astype(F32)
        rows = pl.ds(pl.multiple_of(j * 32, 32), 32)
        along = ky * qy
        for half in range(2):
            lanes = slice(128 * half, 128 * half + 128)
            qx = (lax.broadcasted_iota(jnp.int32, (32, 128), 1) + (128 * half - 128)).astype(F32)
            dot = kx * qx + along
            sign = jnp.where(dot > 0.0, 1.0, -1.0)
            px = kx - sign * qx
            py = ky - sign * qy
            x2 = px * px
            y2 = py * py
            near = x2 + y2
            far = near + 4.0 * jnp.abs(dot)
            phase = chi(px, py, x2, y2, near) - own
            turns = jnp.floor(phase + 0.5)
            f = phase - turns
            z = f * f
            sine = -0.00737043094571435 * z + 0.08214588661112823
            sine = sine * z - 0.5992645293207921
            sine = sine * z + 2.550164039877345
            sine = sine * z - 5.16771278004997
            sine = (sine * z + math.pi) * f
            cosine = 0.0019295743094039 * z - 0.02580689139001406
            cosine = cosine * z + 0.2353306303588935
            cosine = cosine * z - 1.3352627688545893
            cosine = cosine * z + 4.058712126416768
            cosine = cosine * z - 4.934802200544679
            cosine = cosine * z + 1.0
            pair = turns * 0.5
            flip = 1.0 - 4.0 * (pair - jnp.floor(pair))
            flip = jnp.where((near <= BOUND) & (far > BOUND), flip, 0.0)
            w_re[rows, lanes] = flip * sign * cosine
            w_im[rows, lanes] = flip * sine
        return carry

    lax.fori_loop(0, LIVE, one, 0)
    copies[0].wait()
    target = lax.broadcasted_iota(jnp.int32, (256, 32), 0)
    source = lax.broadcasted_iota(jnp.int32, (256, 32), 1)
    repeat = jnp.where(source == target // 16 * 2 + target % 2, 1.0, 0.0).astype(BF)
    table[...] = jnp.dot(repeat, block[...], preferred_element_type=F32).astype(BF)
    copies[1].wait()
    copies[2].wait()


def column_kernel(rows, table, w_re, w_im, inv, out, spec, total):
    held = rows[...].astype(F32).reshape(256, 128).T
    group = (lax.broadcasted_iota(jnp.int32, held.shape, 1) // 2) % 8
    stacked = jnp.concatenate([jnp.where(group == c, held, 0.0) for c in range(7)], axis=0).astype(BF)
    spec[...] = jnp.dot(stacked[: 32 * LIVE], table[...], preferred_element_type=F32)
    total[...] = jnp.zeros((64, BAND), F32)
    for j in range(LIVE):
        part = slice(32 * j, 32 * j + 32)
        s_re, s_im = spec[part, :BAND], spec[part, BAND:]
        a, b = w_re[part, :], w_im[part, :]
        total[j : j + 1, :] = jnp.sum(s_re * a - s_im * b, axis=0, keepdims=True)
        total[32 + j : 33 + j, :] = jnp.sum(s_re * b + s_im * a, axis=0, keepdims=True)
    whole = total[...]
    hi = whole.astype(BF)
    lo = (whole - hi.astype(F32)).astype(BF)
    both = jnp.dot(jnp.concatenate([hi, lo], axis=0), inv[0], preferred_element_type=F32)
    prod = both[:64] + both[64:] + jnp.dot(hi, inv[1], preferred_element_type=F32)
    c_re = prod[:32, :N] - prod[32:, N:]
    c_im = prod[:32, N:] + prod[32:, :N]
    for t in range(4):
        for part, values in enumerate((c_re, c_im)):
            moved = swap_blocks([values[8 * q : 8 * q + 8, 128 * t : 128 * t + 128] for q in range(4)])
            for m in range(4):
                out[4 * (t % 2) + m, t // 2, part] = moved[m].astype(WIRE)


def regroup_kernel(parts, out):
    for half in range(2):
        blocks = []
        for zl in range(2):
            for part in range(2):
                total = parts[zl, half, part].astype(F32)
                for zh in range(1, 4):
                    total = total + parts[2 * zh + zl, half, part].astype(F32)
                blocks += [total if q == 0 else pltpu.roll(total, 128 - 32 * q, 1) for q in range(4)]
        turned = jnp.concatenate(blocks, axis=0).T
        for y in range(8):
            for g in range(4):
                out[16 * g + 8 * half + y] = turned[4 * y : 4 * y + 4].astype(WIRE)


def final_kernel(parts, table, out):
    total = jnp.sum(parts[...].astype(F32).reshape(32, 2, 4, 128), axis=0)
    whole = jnp.concatenate([total[0], total[1]], axis=1)
    hi = whole.astype(BF)
    lo = (whole - hi.astype(F32)).astype(BF)
    both = jnp.dot(jnp.concatenate([hi, lo], axis=0), table[0], preferred_element_type=F32)
    obj = both[:4] + both[4:] + jnp.dot(hi, table[1], preferred_element_type=F32)
    out[0] = obj[:, :128]
    out[1] = obj[:, 128:]


def call(kernel, shapes, specs, operands, scratch=()):
    single = not isinstance(shapes, (list, tuple))
    count = 1 if single else len(shapes)
    spaces = [pltpu.VMEM if spec is KEPT else pltpu.HBM for spec in specs]
    held = [pltpu.with_memory_space_constraint(x, space) for x, space in zip(operands, spaces)]
    return pl.pallas_call(
        kernel,
        out_shape=shapes,
        in_specs=specs,
        out_specs=VMEM if single else [VMEM] * count,
        scratch_shapes=list(scratch),
        compiler_params=pltpu.CompilerParams(vmem_limit_bytes=16 * 2**20),
    )(*held)


def on_device(scan_data, pixel_coords, aberrations):
    row, col, inv, fin = (jnp.asarray(t) for t in tables())
    shape = pltpu.VMEM
    rows = call(row_kernel, shape((4, 4, 16, 128), BF), [VMEM] * 2, (row, scan_data))
    rows = lax.all_to_all(rows, ("zl", "yl"), 0, 0, tiled=True)
    w_re, w_im, table, inv, fin = call(
        weight_kernel,
        [
            shape((32 * LIVE, BAND), F32),
            shape((32 * LIVE, BAND), F32),
            shape((256, N), BF),
            shape((2, 256, 2 * N), BF),
            shape((2, 256, 256), BF),
        ],
        [SMEM, VMEM, ANY, ANY, ANY],
        (aberrations, pixel_coords, col, inv, fin),
        scratch=[pltpu.VMEM((32, N), BF), pltpu.SemaphoreType.DMA((3,))],
    )
    partial = call(
        column_kernel,
        shape((8, 2, 2, 8, 128), WIRE),
        [KEPT] * 5,
        (rows, table, w_re, w_im, inv),
        scratch=[pltpu.VMEM((32 * LIVE, N), F32), pltpu.VMEM((64, BAND), F32)],
    )
    partial = lax.all_to_all(partial, ("zh", "zl"), 0, 0, tiled=True)
    pieces = call(regroup_kernel, shape((64, 4, 128), WIRE), [KEPT], (partial,))
    pieces = lax.all_to_all(pieces, PIX + ("xh", "yh", "yl"), 0, 0, tiled=True)
    return call(final_kernel, jax.ShapeDtypeStruct((2, 4, 128), F32), [KEPT] * 2, (pieces, fin))


def solution(mesh):
    fine = Mesh(mesh.devices.reshape(2, 2, 2, 4, 2, 4, 2), PIX + SCAN)
    placed = (P(PIX, SCAN, None), P(None, PIX), P())
    return jax.shard_map(
        on_device, mesh=fine, in_specs=placed, out_specs=P(None, SCAN, PIX), check_vma=False
    )
```

```python
import functools
import math

import jax
import jax.numpy as jnp
import numpy as np
from jax import lax
from jax.experimental import pallas as pl
from jax.experimental.pallas import tpu as pltpu
from jax.sharding import Mesh, PartitionSpec as P

STEP = 8
N = 512
BAND = 256
BOUND = 40.0 * STEP * STEP
LIVE = 28
VMEM = pl.BlockSpec(memory_space=pltpu.VMEM)
KEPT = pl.BlockSpec(memory_space=pltpu.VMEM)
SMALL = pl.BlockSpec(memory_space=pltpu.SMEM)
ANY = pl.BlockSpec(memory_space=pltpu.HBM)
BF = jnp.bfloat16
F32 = jnp.float32
WIRE = BF
PIX = ("xl", "core")
SCAN = ("xh", "zh", "zl", "yh", "yl")


def angles(k, n):
    return 2.0 * math.pi * np.mod(k * n, N) / N


def split(table):
    hi = table.astype(np.float32).astype(BF)
    lo = (table - hi.astype(np.float64)).astype(np.float32).astype(BF)
    return hi, lo


@functools.lru_cache(None)
def tables():
    jj, m, c = np.meshgrid(np.arange(4), np.arange(4), np.arange(8), indexing="ij")
    ky = (4 * (4 * c + jj) + m)[..., None]
    t = angles(ky, np.arange(N))
    row = np.stack([np.cos(t), -np.sin(t)], axis=3).reshape(256, N).astype(np.float32).astype(BF)
    kx = np.arange(BAND) - BAND // 2
    t = angles(np.arange(N)[:, None], kx[None, :])
    cos, sin = np.cos(t), np.sin(t)
    col = np.stack([np.concatenate([cos, -sin], 1), np.concatenate([sin, cos], 1)], axis=1)
    col = col.reshape(2, 4, 2, 4, 2, 4, 2, 2 * BAND).transpose(0, 1, 3, 2, 4, 5, 6, 7)
    col = col.reshape(32, 32, 2 * BAND).astype(np.float32).astype(BF)
    inv = split(np.concatenate([cos.T, sin.T], 1))
    yl, zl, j = np.meshgrid(np.arange(2), np.arange(2), np.arange(32), indexing="ij")
    ky = 4 * j + 2 * zl + yl
    t = angles(ky[..., None], np.arange(N))
    fold = np.where(ky == 0, 1.0, 2.0)[..., None] / (N * N)
    real = np.where(ky == 0, 1.0, 0.0)[..., None] / (N * N)
    im = np.stack([np.sin(t) * fold, np.cos(t) * fold], axis=2)
    re = np.stack([np.cos(t) * real, -np.sin(t) * real], axis=2)
    fin = np.stack([re, im], axis=4).reshape(256, 2, 4, 128).transpose(2, 0, 1, 3).reshape(4, 256, 256)
    fin = np.stack(split(fin), axis=1)
    return row, col, np.stack(inv), fin


def swap_blocks(parts):
    lane = lax.broadcasted_iota(jnp.int32, parts[0].shape, 1) // 32
    out = []
    for m in range(4):
        acc = parts[0] if m == 0 else pltpu.roll(parts[0], (-32 * m) % 128, 1)
        for q in range(1, 4):
            shift = (32 * (q - m)) % 128
            moved = parts[q] if shift == 0 else pltpu.roll(parts[q], shift, 1)
            acc = jnp.where(lane == q, moved, acc)
        out.append(acc)
    return out


def row_kernel(table, data, out):
    held = data[...].reshape(128, N)
    spec = lax.dot_general(table[...], held, (((1,), (1,)), ((), ())), preferred_element_type=F32)
    parts = [spec[64 * q : 64 * q + 64] for q in range(4)]
    lane = lax.broadcasted_iota(jnp.int32, (64, 128), 1) % 4
    for r in range(4):
        moved = parts[r]
        for q in range(4):
            if q != r:
                moved = jnp.where(lane == q, pltpu.roll(parts[q], (q - r) % 128, 1), moved)
        out[:, r] = moved.reshape(4, 16, 128).astype(BF)


def weight_kernel(coefficients, coords, col, inv, fin, w_re, w_im, table, inv_out, fin_out, block, places, sems):
    here = (lax.axis_index("xh") * 4 + lax.axis_index("zh")) * 4 + lax.axis_index("yh")
    group = lax.axis_index("xl") * 2 + lax.axis_index("core")
    copies = [
        pltpu.make_async_copy(col.at[here], block, sems.at[0]),
        pltpu.make_async_copy(inv, inv_out, sems.at[1]),
        pltpu.make_async_copy(fin.at[group], fin_out, sems.at[2]),
    ]
    for copy in copies:
        copy.start()

    a0 = coefficients[0] / (BOUND * math.pi)
    a1 = coefficients[1] / (BOUND * math.pi)
    a2 = coefficients[2] * 2.0 / (BOUND * math.pi)
    a3 = coefficients[3] / (BOUND * BOUND * math.pi)
    first = (2 * lax.axis_index("zl") + lax.axis_index("yl")).astype(F32)

    def chi(px, py, x2, y2, r2):
        return r2 * (a0 + a3 * r2) + (a1 * (x2 - y2) + a2 * (px * py))

    centre = coords[...].astype(F32) * float(STEP)
    source = lax.broadcasted_iota(jnp.int32, (32, 128), 0)
    target = lax.broadcasted_iota(jnp.int32, (32, 128), 1)
    centre = jnp.dot(centre, jnp.where(source == target // 4, 1.0, 0.0), preferred_element_type=F32)
    for n in range(2):
        places[n] = jnp.broadcast_to(centre[n : n + 1], (128, 128)).T
    wide, tall = places[0], places[1]
    places[2] = chi(wide, tall, wide * wide, tall * tall, wide * wide + tall * tall)
    step = first + 4.0 * (lax.broadcasted_iota(jnp.int32, (32, 128), 0) % 4).astype(F32)

    def one(n, carry):
        qy = step + 16.0 * (n // 4).astype(F32)
        here = pl.ds(pl.multiple_of(n % 4 * 32, 32), 32)
        kx, ky, own = places[0, here], places[1, here], places[2, here]
        rows = pl.ds(pl.multiple_of(n * 32, 32), 32)
        along = ky * qy
        for half in range(2):
            lanes = slice(128 * half, 128 * half + 128)
            qx = (lax.broadcasted_iota(jnp.int32, (32, 128), 1) + (128 * half - 128)).astype(F32)
            dot = kx * qx + along
            sign = jnp.where(dot > 0.0, 1.0, -1.0)
            px = kx - sign * qx
            py = ky - sign * qy
            x2 = px * px
            y2 = py * py
            near = x2 + y2
            far = near + 4.0 * jnp.abs(dot)
            phase = chi(px, py, x2, y2, near) - own
            turns = jnp.floor(phase + 0.5)
            f = phase - turns
            z = f * f
            sine = -0.00737043094571435 * z + 0.08214588661112823
            sine = sine * z - 0.5992645293207921
            sine = sine * z + 2.550164039877345
            sine = sine * z - 5.16771278004997
            sine = (sine * z + math.pi) * f
            cosine = 0.0019295743094039 * z - 0.02580689139001406
            cosine = cosine * z + 0.2353306303588935
            cosine = cosine * z - 1.3352627688545893
            cosine = cosine * z + 4.058712126416768
            cosine = cosine * z - 4.934802200544679
            cosine = cosine * z + 1.0
            pair = turns * 0.5
            flip = 1.0 - 4.0 * (pair - jnp.floor(pair))
            flip = jnp.where((near <= BOUND) & (far > BOUND), flip, 0.0)
            w_re[rows, lanes] = flip * sign * cosine
            w_im[rows, lanes] = flip * sine
        return carry

    lax.fori_loop(0, LIVE, one, 0)
    copies[0].wait()
    target = lax.broadcasted_iota(jnp.int32, (256, 32), 0)
    source = lax.broadcasted_iota(jnp.int32, (256, 32), 1)
    repeat = jnp.where(source == target // 16 * 2 + target % 2, 1.0, 0.0).astype(BF)
    table[...] = jnp.dot(repeat, block[...], preferred_element_type=F32).astype(BF)
    copies[1].wait()
    copies[2].wait()


def column_kernel(rows, table, w_re, w_im, inv, out, spec, total):
    held = rows[...].astype(F32).reshape(256, 128).T
    group = (lax.broadcasted_iota(jnp.int32, held.shape, 1) // 2) % 8
    stacked = jnp.concatenate([jnp.where(group == c, held, 0.0) for c in range(LIVE // 4)], axis=0).astype(BF)
    spec[...] = jnp.dot(stacked, table[...], preferred_element_type=F32)
    total[...] = jnp.zeros((64, BAND), F32)
    for c in range(LIVE // 4):
        part = slice(128 * c, 128 * c + 128)
        s_re, s_im = spec[part, :BAND], spec[part, BAND:]
        a, b = w_re[part, :], w_im[part, :]
        for n, z in enumerate((s_re * a - s_im * b, s_re * b + s_im * a)):
            pair = jnp.sum(z.reshape(16, 8, BAND), axis=0)
            total[32 * n + 4 * c : 32 * n + 4 * c + 4, :] = pair[:4] + pair[4:]
    whole = total[...]
    hi = whole.astype(BF)
    lo = (whole - hi.astype(F32)).astype(BF)
    both = jnp.dot(jnp.concatenate([hi, lo], axis=0), inv[0], preferred_element_type=F32)
    prod = both[:64] + both[64:] + jnp.dot(hi, inv[1], preferred_element_type=F32)
    c_re = prod[:32, :N] - prod[32:, N:]
    c_im = prod[:32, N:] + prod[32:, :N]
    for t in range(4):
        for part, values in enumerate((c_re, c_im)):
            moved = swap_blocks([values[8 * q : 8 * q + 8, 128 * t : 128 * t + 128] for q in range(4)])
            for m in range(4):
                for core in range(2):
                    out[2 * (4 * (t % 2) + m) + core, t // 2, part] = moved[m].astype(WIRE)


def regroup_kernel(parts, out):
    for half in range(2):
        blocks = []
        for zl in range(2):
            for part in range(2):
                total = parts[2 * zl, half, part].astype(F32) + parts[2 * zl + 1, half, part].astype(F32)
                for zh in range(1, 4):
                    for core in range(2):
                        total = total + parts[2 * (2 * zh + zl) + core, half, part].astype(F32)
                blocks += [total if q == 0 else pltpu.roll(total, 128 - 32 * q, 1) for q in range(4)]
        turned = jnp.concatenate(blocks, axis=0).T
        for y in range(8):
            for g in range(2):
                out[16 * g + 8 * half + y] = turned[4 * y : 4 * y + 4].astype(WIRE)


def final_kernel(parts, table, out):
    total = jnp.sum(parts[...].astype(F32).reshape(16, 2, 4, 128), axis=0)
    whole = jnp.concatenate([total[0], total[1]], axis=1)
    hi = whole.astype(BF)
    lo = (whole - hi.astype(F32)).astype(BF)
    both = jnp.dot(jnp.concatenate([hi, lo], axis=0), table[0], preferred_element_type=F32)
    obj = both[:4] + both[4:] + jnp.dot(hi, table[1], preferred_element_type=F32)
    out[0] = obj[:, :128]
    out[1] = obj[:, 128:]


def call(kernel, shapes, specs, operands, scratch=()):
    single = not isinstance(shapes, (list, tuple))
    count = 1 if single else len(shapes)
    spaces = [pltpu.VMEM if spec is KEPT else pltpu.SMEM if spec is SMALL else pltpu.HBM for spec in specs]
    held = [pltpu.with_memory_space_constraint(x, space) for x, space in zip(operands, spaces)]
    return pl.pallas_call(
        kernel,
        out_shape=shapes,
        in_specs=specs,
        out_specs=VMEM if single else [VMEM] * count,
        scratch_shapes=list(scratch),
        compiler_params=pltpu.CompilerParams(vmem_limit_bytes=16 * 2**20),
    )(*held)


def on_device(scan_data, pixel_coords, aberrations):
    row, col, inv, fin = (jnp.asarray(t) for t in tables())
    shape = pltpu.VMEM
    rows = call(row_kernel, shape((4, 4, 16, 128), BF), [VMEM] * 2, (row, scan_data))
    rows = lax.all_to_all(rows, ("zl", "yl"), 0, 0, tiled=True)
    w_re, w_im, table, inv, fin = call(
        weight_kernel,
        [
            shape((32 * LIVE, BAND), F32),
            shape((32 * LIVE, BAND), F32),
            shape((256, N), BF),
            shape((2, 256, 2 * N), BF),
            shape((2, 256, 256), BF),
        ],
        [SMALL, KEPT, ANY, ANY, ANY],
        (aberrations, pixel_coords, col, inv, fin),
        scratch=[pltpu.VMEM((32, N), BF), pltpu.VMEM((3, 128, 128), F32), pltpu.SemaphoreType.DMA((3,))],
    )
    partial = call(
        column_kernel,
        shape((16, 2, 2, 8, 128), WIRE),
        [KEPT] * 5,
        (rows, table, w_re, w_im, inv),
        scratch=[pltpu.VMEM((32 * LIVE, N), F32), pltpu.VMEM((64, BAND), F32)],
    )
    partial = lax.all_to_all(partial, ("zh", "zl", "core"), 0, 0, tiled=True)
    pieces = call(regroup_kernel, shape((32, 4, 128), WIRE), [KEPT], (partial,))
    pieces = lax.all_to_all(pieces, ("xl", "xh", "yh", "yl"), 0, 0, tiled=True)
    return call(final_kernel, jax.ShapeDtypeStruct((2, 4, 128), F32), [KEPT] * 2, (pieces, fin))


def solution(mesh):
    fine = Mesh(mesh.devices.reshape(2, 2, 2, 4, 2, 4, 2), PIX + SCAN)
    placed = (P(PIX, SCAN, None), P(None, PIX), P())
    return jax.shard_map(
        on_device, mesh=fine, in_specs=placed, out_specs=P(None, SCAN, PIX), check_vma=False
    )
```

```python
import functools
import math

import jax
import jax.numpy as jnp
import numpy as np
from jax import lax
from jax.experimental import pallas as pl
from jax.experimental.pallas import tpu as pltpu
from jax.sharding import Mesh, PartitionSpec as P

STEP = 8
N = 512
BAND = 256
BOUND = 40.0 * STEP * STEP
VMEM = pl.BlockSpec(memory_space=pltpu.VMEM)
KEPT = pl.BlockSpec(memory_space=pltpu.VMEM)
SMALL = pl.BlockSpec(memory_space=pltpu.SMEM)
ANY = pl.BlockSpec(memory_space=pltpu.HBM)
BF = jnp.bfloat16
F32 = jnp.float32


def angles(k, n):
    return 2.0 * math.pi * np.mod(k * n, N) / N


def split(table):
    hi = table.astype(np.float32).astype(BF)
    lo = (table - hi.astype(np.float64)).astype(np.float32).astype(BF)
    return hi, lo


@functools.lru_cache(None)
def tables():
    jj, yy, c = np.meshgrid(np.arange(4), np.arange(8), np.arange(4), indexing="ij")
    ky = (8 * (4 * c + jj) + yy)[..., None]
    t = angles(ky, np.arange(N))
    row = np.stack([np.cos(t), -np.sin(t)], axis=3).reshape(256, N).astype(np.float32).astype(BF)
    kx = np.arange(BAND) - BAND // 2
    t = angles(np.arange(N)[:, None], kx[None, :])
    cos, sin = np.cos(t), np.sin(t)
    col = np.stack([np.concatenate([cos, -sin], 1), np.concatenate([sin, cos], 1)], axis=1)
    col = col.reshape(16, 64, 2 * BAND).astype(np.float32).astype(BF)
    place = (np.arange(16)[:, None, None] * 32 + np.arange(4)[:, None] + 4 * np.arange(8)).reshape(-1)
    inv = split(np.concatenate([cos.T[:, place], sin.T[:, place]], 1))
    yy, j = np.meshgrid(np.arange(8), np.arange(16), indexing="ij")
    ky = 8 * j + yy
    t = angles(ky[..., None], np.arange(N))
    fold = np.where(ky == 0, 1.0, 2.0)[..., None] / (N * N)
    real = np.where(ky == 0, 1.0, 0.0)[..., None] / (N * N)
    im = np.stack([np.sin(t) * fold, np.cos(t) * fold], axis=1)
    re = np.stack([np.cos(t) * real, -np.sin(t) * real], axis=1)
    fin = np.stack([re, im], axis=3).reshape(256, 2, 4, 128).transpose(2, 0, 1, 3).reshape(4, 256, 256)
    fin = np.stack(split(fin), axis=1)
    return row, col, np.stack(inv), fin


def swap_blocks(parts):
    lane = lax.broadcasted_iota(jnp.int32, parts[0].shape, 1) // 32
    out = []
    for m in range(4):
        acc = parts[0] if m == 0 else pltpu.roll(parts[0], (-32 * m) % 128, 1)
        for q in range(1, 4):
            shift = (32 * (q - m)) % 128
            moved = parts[q] if shift == 0 else pltpu.roll(parts[q], shift, 1)
            acc = jnp.where(lane == q, moved, acc)
        out.append(acc)
    return out


def row_kernel(table, data, out):
    held = data[...].reshape(128, N)
    spec = lax.dot_general(table[...], held, (((1,), (1,)), ((), ())), preferred_element_type=F32)
    parts = [spec[64 * q : 64 * q + 64] for q in range(4)]
    lane = lax.broadcasted_iota(jnp.int32, (64, 128), 1) % 4
    for r in range(4):
        moved = parts[r]
        for q in range(4):
            if q != r:
                moved = jnp.where(lane == q, pltpu.roll(parts[q], (q - r) % 128, 1), moved)
        out[:, r] = moved.reshape(8, 8, 128).astype(BF)


def weight_kernel(coefficients, coords, col, inv, fin, w_re, w_im, table, inv_out, fin_out, block, places, sems):
    here = lax.axis_index("xh") * 8 + lax.axis_index("z")
    group = lax.axis_index("xl") * 2 + lax.axis_index("core")
    copies = [
        pltpu.make_async_copy(col.at[here], block, sems.at[0]),
        pltpu.make_async_copy(inv, inv_out, sems.at[1]),
        pltpu.make_async_copy(fin.at[group], fin_out, sems.at[2]),
    ]
    for copy in copies:
        copy.start()

    a0 = coefficients[0] / (BOUND * math.pi)
    a1 = coefficients[1] / (BOUND * math.pi)
    a2 = coefficients[2] * 2.0 / (BOUND * math.pi)
    a3 = coefficients[3] / (BOUND * BOUND * math.pi)
    first = lax.axis_index("y").astype(F32)

    def chi(px, py, x2, y2, r2):
        return r2 * (a0 + a3 * r2) + (a1 * (x2 - y2) + a2 * (px * py))

    centre = coords[...].astype(F32) * float(STEP)
    source = lax.broadcasted_iota(jnp.int32, (32, 128), 0)
    target = lax.broadcasted_iota(jnp.int32, (32, 128), 1)
    centre = jnp.dot(centre, jnp.where(source == target // 4, 1.0, 0.0), preferred_element_type=F32)
    for n in range(2):
        places[n] = jnp.broadcast_to(centre[n : n + 1], (128, 128)).T
    wide, tall = places[0], places[1]
    places[2] = chi(wide, tall, wide * wide, tall * tall, wide * wide + tall * tall)
    step = first + 8.0 * (lax.broadcasted_iota(jnp.int32, (32, 128), 0) % 4).astype(F32)

    def one(n, carry):
        qy = step + 32.0 * (n // 4).astype(F32)
        here = pl.ds(pl.multiple_of(n % 4 * 32, 32), 32)
        kx, ky, own = places[0, here], places[1, here], places[2, here]
        rows = pl.ds(pl.multiple_of(n * 32, 32), 32)
        along = ky * qy
        for half in range(2):
            lanes = slice(128 * half, 128 * half + 128)
            qx = (lax.broadcasted_iota(jnp.int32, (32, 128), 1) + (128 * half - 128)).astype(F32)
            dot = kx * qx + along
            sign = jnp.where(dot > 0.0, 1.0, -1.0)
            px = kx - sign * qx
            py = ky - sign * qy
            x2 = px * px
            y2 = py * py
            near = x2 + y2
            far = near + 4.0 * jnp.abs(dot)
            phase = chi(px, py, x2, y2, near) - own
            turns = jnp.floor(phase + 0.5)
            f = phase - turns
            z = f * f
            sine = -0.00737043094571435 * z + 0.08214588661112823
            sine = sine * z - 0.5992645293207921
            sine = sine * z + 2.550164039877345
            sine = sine * z - 5.16771278004997
            sine = (sine * z + math.pi) * f
            cosine = 0.0019295743094039 * z - 0.02580689139001406
            cosine = cosine * z + 0.2353306303588935
            cosine = cosine * z - 1.3352627688545893
            cosine = cosine * z + 4.058712126416768
            cosine = cosine * z - 4.934802200544679
            cosine = cosine * z + 1.0
            pair = turns * 0.5
            flip = 1.0 - 4.0 * (pair - jnp.floor(pair))
            flip = jnp.where((near <= BOUND) & (far > BOUND), flip, 0.0)
            w_re[rows, lanes] = flip * sign * cosine
            w_im[rows, lanes] = flip * sine
        return carry

    lax.fori_loop(0, 16, one, 0)
    copies[0].wait()
    target = lax.broadcasted_iota(jnp.int32, (256, 64), 0)
    source = lax.broadcasted_iota(jnp.int32, (256, 64), 1)
    repeat = jnp.where(source == target // 8 * 2 + target % 2, 1.0, 0.0).astype(BF)
    table[...] = jnp.dot(repeat, block[...], preferred_element_type=F32).astype(BF)
    copies[1].wait()
    copies[2].wait()


def column_kernel(rows, table, w_re, w_im, inv, out, spec, total):
    held = rows[...].astype(F32).reshape(256, 128).T
    group = (lax.broadcasted_iota(jnp.int32, held.shape, 1) // 2) % 4
    stacked = jnp.concatenate([jnp.where(group == c, held, 0.0) for c in range(4)], axis=0).astype(BF)
    spec[...] = jnp.dot(stacked, table[...], preferred_element_type=F32)
    for c in range(4):
        part = slice(128 * c, 128 * c + 128)
        s_re, s_im = spec[part, :BAND], spec[part, BAND:]
        a, b = w_re[part, :], w_im[part, :]
        for n, z in enumerate((s_re * a - s_im * b, s_re * b + s_im * a)):
            pair = jnp.sum(z.reshape(16, 8, BAND), axis=0)
            total[16 * n + 4 * c : 16 * n + 4 * c + 4, :] = pair[:4] + pair[4:]
    whole = total[...]
    hi = whole.astype(BF)
    lo = (whole - hi.astype(F32)).astype(BF)
    both = jnp.dot(jnp.concatenate([hi, lo], axis=0), inv[0], preferred_element_type=F32)
    prod = both[:32] + both[32:] + jnp.dot(hi, inv[1], preferred_element_type=F32)
    c_re = prod[:16, :N] - prod[16:, N:]
    c_im = prod[:16, N:] + prod[16:, :N]
    quarters = [c_re[:8], c_re[8:], c_im[:8], c_im[8:]]
    for t in range(4):
        moved = swap_blocks([v[:, 128 * t : 128 * t + 128] for v in quarters])
        for m in range(4):
            for core in range(2):
                out[2 * (4 * (t % 2) + m) + core, t // 2] = moved[m]


def regroup_kernel(parts, out):
    blocks = []
    for half in range(2):
        total = jnp.sum(parts[:, half], axis=0)
        blocks += [total if q == 0 else pltpu.roll(total, 128 - 32 * q, 1) for q in range(4)]
    turned = jnp.concatenate(blocks * 2, axis=0).T
    lane = lax.broadcasted_iota(jnp.int32, (8, 128), 1) // 32
    for half in range(2):
        acc = jnp.zeros((8, 128), F32)
        for r in range(4):
            piece = turned[8 * r : 8 * r + 8]
            shift = 32 * (r - half) % 128
            acc = jnp.where(lane == r, piece if shift == 0 else pltpu.roll(piece, shift, 1), acc)
        for g in range(2):
            out[16 * g + 8 * half : 16 * g + 8 * half + 8] = acc


def final_kernel(parts, table, out):
    total = parts[0:8]
    for n in range(1, 4):
        total = total + parts[8 * n : 8 * n + 8]
    turns = [total if s == 0 else pltpu.roll(total, 32 * s, 1) for s in range(4)]
    row = lax.broadcasted_iota(jnp.int32, (8, 128), 0) % 4
    lane = lax.broadcasted_iota(jnp.int32, (8, 128), 1) // 32
    rows = []
    for r in range(4):
        spread = jnp.zeros((8, 128), F32)
        for a in range(4):
            spread = jnp.where((row == a) & (lane == a), turns[(a - r) % 4], spread)
        low = jnp.sum(spread[:4], axis=0, keepdims=True)
        high = jnp.sum(spread[4:], axis=0, keepdims=True)
        rows.append(jnp.concatenate([low, high], axis=1))
    whole = jnp.concatenate(rows, axis=0)
    hi = whole.astype(BF)
    lo = (whole - hi.astype(F32)).astype(BF)
    both = jnp.dot(jnp.concatenate([hi, lo], axis=0), table[0], preferred_element_type=F32)
    obj = both[:4] + both[4:] + jnp.dot(hi, table[1], preferred_element_type=F32)
    out[0] = obj[:, :128]
    out[1] = obj[:, 128:]


def call(kernel, shapes, specs, operands, scratch=()):
    single = not isinstance(shapes, (list, tuple))
    count = 1 if single else len(shapes)
    spaces = [pltpu.VMEM if spec is KEPT else pltpu.SMEM if spec is SMALL else pltpu.HBM for spec in specs]
    held = [pltpu.with_memory_space_constraint(x, space) for x, space in zip(operands, spaces)]
    return pl.pallas_call(
        kernel,
        out_shape=shapes,
        in_specs=specs,
        out_specs=VMEM if single else [VMEM] * count,
        scratch_shapes=list(scratch),
        compiler_params=pltpu.CompilerParams(vmem_limit_bytes=16 * 2**20),
    )(*held)


def on_device(scan_data, pixel_coords, aberrations):
    row, col, inv, fin = (jnp.asarray(t) for t in tables())
    shape = pltpu.VMEM
    rows = call(row_kernel, shape((8, 4, 8, 128), BF), [VMEM] * 2, (row, scan_data))
    rows = lax.all_to_all(rows, "y", 0, 0, tiled=True)
    w_re, w_im, table, inv, fin = call(
        weight_kernel,
        [
            shape((512, BAND), F32),
            shape((512, BAND), F32),
            shape((256, N), BF),
            shape((2, 256, 2 * N), BF),
            shape((2, 256, 256), BF),
        ],
        [SMALL, KEPT, ANY, ANY, ANY],
        (aberrations, pixel_coords, col, inv, fin),
        scratch=[pltpu.VMEM((64, N), BF), pltpu.VMEM((3, 128, 128), F32), pltpu.SemaphoreType.DMA((3,))],
    )
    partial = call(
        column_kernel,
        shape((16, 2, 8, 128), F32),
        [KEPT] * 5,
        (rows, table, w_re, w_im, inv),
        scratch=[pltpu.VMEM((512, N), F32), pltpu.VMEM((32, BAND), F32)],
    )
    partial = lax.all_to_all(partial, ("z", "core"), 0, 0, tiled=True)
    pieces = call(regroup_kernel, shape((32, 128), F32), [KEPT], (partial,))
    pieces = lax.all_to_all(pieces.reshape(32, 1, 128), ("xl", "xh", "y"), 0, 0, tiled=True)
    return call(final_kernel, jax.ShapeDtypeStruct((2, 4, 128), F32), [KEPT] * 2, (pieces.reshape(32, 128), fin))


def solution(mesh):
    axes = ("xl", "core", "xh", "z", "y")
    fine = Mesh(mesh.devices.reshape(2, 2, 2, 8, 8), axes)
    pix, scan = ("xl", "core"), ("xh", "z", "y")
    placed = (P(pix, scan, None), P(None, pix), P())
    return jax.shard_map(
        on_device, mesh=fine, in_specs=placed, out_specs=P(None, scan, pix), check_vma=False
    )
```

```python
import functools
import math

import jax
import jax.numpy as jnp
import numpy as np
from jax import lax
from jax.experimental import pallas as pl
from jax.experimental.pallas import tpu as pltpu
from jax.sharding import Mesh, PartitionSpec as P

STEP = 8
N = 512
BAND = 256
BOUND = 40.0 * STEP * STEP
VMEM = pl.BlockSpec(memory_space=pltpu.VMEM)
KEPT = pl.BlockSpec(memory_space=pltpu.VMEM)
SMALL = pl.BlockSpec(memory_space=pltpu.SMEM)
ANY = pl.BlockSpec(memory_space=pltpu.HBM)
BF = jnp.bfloat16
F32 = jnp.float32
FIRST, SECOND = "z", "y"
STRIDE = {"z": 32, "y": 4}
PLACES = 256 * np.arange(2)[:, None, None, None] + STRIDE[SECOND] * np.arange(8)[:, None, None]


def angles(k, n):
    return 2.0 * math.pi * np.mod(k * n, N) / N


def split(table):
    hi = table.astype(np.float32).astype(BF)
    lo = (table - hi.astype(np.float64)).astype(np.float32).astype(BF)
    return hi, lo


@functools.lru_cache(None)
def tables():
    jj, yy, c = np.meshgrid(np.arange(4), np.arange(8), np.arange(4), indexing="ij")
    ky = (8 * (4 * c + jj) + yy)[..., None]
    t = angles(ky, np.arange(N))
    row = np.stack([np.cos(t), -np.sin(t)], axis=3).reshape(256, N).astype(np.float32).astype(BF)
    kx = np.arange(BAND) - BAND // 2
    t = angles(np.arange(N)[:, None], kx[None, :])
    cos, sin = np.cos(t), np.sin(t)
    col = np.stack([np.concatenate([cos, -sin], 1), np.concatenate([sin, cos], 1)], axis=1)
    place = (PLACES + STRIDE[FIRST] * np.arange(8)[:, None] + np.arange(4)).reshape(-1)
    col = col[place].reshape(16, 64, 2 * BAND).astype(np.float32).astype(BF)
    place = (PLACES + np.arange(4)[:, None] + STRIDE[FIRST] * np.arange(8)).reshape(-1)
    inv = split(np.concatenate([cos.T[:, place], sin.T[:, place]], 1))
    yy, j = np.meshgrid(np.arange(8), np.arange(16), indexing="ij")
    ky = 8 * j + yy
    t = angles(ky[..., None], np.arange(N))
    fold = np.where(ky == 0, 1.0, 2.0)[..., None] / (N * N)
    real = np.where(ky == 0, 1.0, 0.0)[..., None] / (N * N)
    im = np.stack([np.sin(t) * fold, np.cos(t) * fold], axis=1)
    re = np.stack([np.cos(t) * real, -np.sin(t) * real], axis=1)
    fin = np.stack([re, im], axis=3).reshape(256, 2, 4, 128).transpose(2, 0, 1, 3).reshape(4, 256, 256)
    fin = np.stack(split(fin), axis=1)
    return row, col, np.stack(inv), fin


def swap_blocks(parts):
    lane = lax.broadcasted_iota(jnp.int32, parts[0].shape, 1) // 32
    out = []
    for m in range(4):
        acc = parts[0] if m == 0 else pltpu.roll(parts[0], (-32 * m) % 128, 1)
        for q in range(1, 4):
            shift = (32 * (q - m)) % 128
            moved = parts[q] if shift == 0 else pltpu.roll(parts[q], shift, 1)
            acc = jnp.where(lane == q, moved, acc)
        out.append(acc)
    return out


def row_kernel(table, data, out):
    held = data[...].reshape(128, N)
    spec = lax.dot_general(table[...], held, (((1,), (1,)), ((), ())), preferred_element_type=F32)
    parts = [spec[64 * q : 64 * q + 64] for q in range(4)]
    lane = lax.broadcasted_iota(jnp.int32, (64, 128), 1) % 4
    for r in range(4):
        moved = parts[r]
        for q in range(4):
            if q != r:
                moved = jnp.where(lane == q, pltpu.roll(parts[q], (q - r) % 128, 1), moved)
        out[:, r] = moved.reshape(8, 8, 128).astype(BF)


def weight_kernel(coefficients, coords, col, inv, fin, w_re, w_im, table, inv_out, fin_out, block, places, sems):
    here = lax.axis_index("xh") * 8 + lax.axis_index(SECOND)
    group = lax.axis_index("xl") * 2 + lax.axis_index("core")
    copies = [
        pltpu.make_async_copy(col.at[here], block, sems.at[0]),
        pltpu.make_async_copy(inv, inv_out, sems.at[1]),
        pltpu.make_async_copy(fin.at[group], fin_out, sems.at[2]),
    ]
    for copy in copies:
        copy.start()

    a0 = coefficients[0] / (BOUND * math.pi)
    a1 = coefficients[1] / (BOUND * math.pi)
    a2 = coefficients[2] * 2.0 / (BOUND * math.pi)
    a3 = coefficients[3] / (BOUND * BOUND * math.pi)
    first = lax.axis_index(FIRST).astype(F32)

    def chi(px, py, x2, y2, r2):
        return r2 * (a0 + a3 * r2) + (a1 * (x2 - y2) + a2 * (px * py))

    centre = coords[...].astype(F32) * float(STEP)
    source = lax.broadcasted_iota(jnp.int32, (32, 128), 0)
    target = lax.broadcasted_iota(jnp.int32, (32, 128), 1)
    centre = jnp.dot(centre, jnp.where(source == target // 4, 1.0, 0.0), preferred_element_type=F32)
    for n in range(2):
        places[n] = jnp.broadcast_to(centre[n : n + 1], (128, 128)).T
    wide, tall = places[0], places[1]
    places[2] = chi(wide, tall, wide * wide, tall * tall, wide * wide + tall * tall)
    step = first + 8.0 * (lax.broadcasted_iota(jnp.int32, (32, 128), 0) % 4).astype(F32)

    def one(n, carry):
        qy = step + 32.0 * (n // 4).astype(F32)
        here = pl.ds(pl.multiple_of(n % 4 * 32, 32), 32)
        kx, ky, own = places[0, here], places[1, here], places[2, here]
        rows = pl.ds(pl.multiple_of(n * 32, 32), 32)
        along = ky * qy
        for half in range(2):
            lanes = slice(128 * half, 128 * half + 128)
            qx = (lax.broadcasted_iota(jnp.int32, (32, 128), 1) + (128 * half - 128)).astype(F32)
            dot = kx * qx + along
            sign = jnp.where(dot > 0.0, 1.0, -1.0)
            px = kx - sign * qx
            py = ky - sign * qy
            x2 = px * px
            y2 = py * py
            near = x2 + y2
            far = near + 4.0 * jnp.abs(dot)
            phase = chi(px, py, x2, y2, near) - own
            turns = jnp.floor(phase + 0.5)
            f = phase - turns
            z = f * f
            sine = -0.00737043094571435 * z + 0.08214588661112823
            sine = sine * z - 0.5992645293207921
            sine = sine * z + 2.550164039877345
            sine = sine * z - 5.16771278004997
            sine = (sine * z + math.pi) * f
            cosine = 0.0019295743094039 * z - 0.02580689139001406
            cosine = cosine * z + 0.2353306303588935
            cosine = cosine * z - 1.3352627688545893
            cosine = cosine * z + 4.058712126416768
            cosine = cosine * z - 4.934802200544679
            cosine = cosine * z + 1.0
            pair = turns * 0.5
            flip = 1.0 - 4.0 * (pair - jnp.floor(pair))
            flip = jnp.where((near <= BOUND) & (far > BOUND), flip, 0.0)
            w_re[rows, lanes] = flip * sign * cosine
            w_im[rows, lanes] = flip * sine
        return carry

    lax.fori_loop(0, 16, one, 0)
    copies[0].wait()
    target = lax.broadcasted_iota(jnp.int32, (256, 64), 0)
    source = lax.broadcasted_iota(jnp.int32, (256, 64), 1)
    repeat = jnp.where(source == target // 8 * 2 + target % 2, 1.0, 0.0).astype(BF)
    table[...] = jnp.dot(repeat, block[...], preferred_element_type=F32).astype(BF)
    copies[1].wait()
    copies[2].wait()


def column_kernel(rows, table, w_re, w_im, inv, out, spec, total):
    held = rows[...].astype(F32).reshape(256, 128).T
    group = (lax.broadcasted_iota(jnp.int32, held.shape, 1) // 2) % 4
    stacked = jnp.concatenate([jnp.where(group == c, held, 0.0) for c in range(4)], axis=0).astype(BF)
    spec[...] = jnp.dot(stacked, table[...], preferred_element_type=F32)
    for c in range(4):
        part = slice(128 * c, 128 * c + 128)
        s_re, s_im = spec[part, :BAND], spec[part, BAND:]
        a, b = w_re[part, :], w_im[part, :]
        for n, z in enumerate((s_re * a - s_im * b, s_re * b + s_im * a)):
            pair = jnp.sum(z.reshape(16, 8, BAND), axis=0)
            total[16 * n + 4 * c : 16 * n + 4 * c + 4, :] = pair[:4] + pair[4:]
    whole = total[...]
    hi = whole.astype(BF)
    lo = (whole - hi.astype(F32)).astype(BF)
    both = jnp.dot(jnp.concatenate([hi, lo], axis=0), inv[0], preferred_element_type=F32)
    prod = both[:32] + both[32:] + jnp.dot(hi, inv[1], preferred_element_type=F32)
    c_re = prod[:16, :N] - prod[16:, N:]
    c_im = prod[:16, N:] + prod[16:, :N]
    quarters = [c_re[:8], c_re[8:], c_im[:8], c_im[8:]]
    for t in range(4):
        moved = swap_blocks([v[:, 128 * t : 128 * t + 128] for v in quarters])
        for m in range(4):
            for core in range(2):
                out[2 * (4 * (t % 2) + m) + core, t // 2] = moved[m]


def regroup_kernel(parts, out):
    blocks = []
    for half in range(2):
        total = jnp.sum(parts[:, half], axis=0)
        blocks += [total if q == 0 else pltpu.roll(total, 128 - 32 * q, 1) for q in range(4)]
    turned = jnp.concatenate(blocks * 2, axis=0).T
    lane = lax.broadcasted_iota(jnp.int32, (8, 128), 1) // 32
    for half in range(2):
        acc = jnp.zeros((8, 128), F32)
        for r in range(4):
            piece = turned[8 * r : 8 * r + 8]
            shift = 32 * (r - half) % 128
            acc = jnp.where(lane == r, piece if shift == 0 else pltpu.roll(piece, shift, 1), acc)
        for g in range(2):
            out[16 * g + 8 * half : 16 * g + 8 * half + 8] = acc


def final_kernel(parts, table, out):
    total = parts[0:8]
    for n in range(1, 4):
        total = total + parts[8 * n : 8 * n + 8]
    turns = [total if s == 0 else pltpu.roll(total, 32 * s, 1) for s in range(4)]
    row = lax.broadcasted_iota(jnp.int32, (8, 128), 0) % 4
    lane = lax.broadcasted_iota(jnp.int32, (8, 128), 1) // 32
    rows = []
    for r in range(4):
        spread = jnp.zeros((8, 128), F32)
        for a in range(4):
            spread = jnp.where((row == a) & (lane == a), turns[(a - r) % 4], spread)
        low = jnp.sum(spread[:4], axis=0, keepdims=True)
        high = jnp.sum(spread[4:], axis=0, keepdims=True)
        rows.append(jnp.concatenate([low, high], axis=1))
    whole = jnp.concatenate(rows, axis=0)
    hi = whole.astype(BF)
    lo = (whole - hi.astype(F32)).astype(BF)
    both = jnp.dot(jnp.concatenate([hi, lo], axis=0), table[0], preferred_element_type=F32)
    obj = both[:4] + both[4:] + jnp.dot(hi, table[1], preferred_element_type=F32)
    out[0] = obj[:, :128]
    out[1] = obj[:, 128:]


def call(kernel, shapes, specs, operands, scratch=()):
    single = not isinstance(shapes, (list, tuple))
    count = 1 if single else len(shapes)
    spaces = [pltpu.VMEM if spec is KEPT else pltpu.SMEM if spec is SMALL else pltpu.HBM for spec in specs]
    held = [pltpu.with_memory_space_constraint(x, space) for x, space in zip(operands, spaces)]
    return pl.pallas_call(
        kernel,
        out_shape=shapes,
        in_specs=specs,
        out_specs=VMEM if single else [VMEM] * count,
        scratch_shapes=list(scratch),
        compiler_params=pltpu.CompilerParams(vmem_limit_bytes=16 * 2**20),
    )(*held)


def on_device(scan_data, pixel_coords, aberrations):
    row, col, inv, fin = (jnp.asarray(t) for t in tables())
    shape = pltpu.VMEM
    rows = call(row_kernel, shape((8, 4, 8, 128), BF), [VMEM] * 2, (row, scan_data))
    rows = lax.all_to_all(rows, FIRST, 0, 0, tiled=True)
    w_re, w_im, table, inv, fin = call(
        weight_kernel,
        [
            shape((512, BAND), F32),
            shape((512, BAND), F32),
            shape((256, N), BF),
            shape((2, 256, 2 * N), BF),
            shape((2, 256, 256), BF),
        ],
        [SMALL, KEPT, ANY, ANY, ANY],
        (aberrations, pixel_coords, col, inv, fin),
        scratch=[pltpu.VMEM((64, N), BF), pltpu.VMEM((3, 128, 128), F32), pltpu.SemaphoreType.DMA((3,))],
    )
    partial = call(
        column_kernel,
        shape((16, 2, 8, 128), F32),
        [KEPT] * 5,
        (rows, table, w_re, w_im, inv),
        scratch=[pltpu.VMEM((512, N), F32), pltpu.VMEM((32, BAND), F32)],
    )
    partial = lax.all_to_all(partial, (SECOND, "core"), 0, 0, tiled=True)
    pieces = call(regroup_kernel, shape((32, 128), F32), [KEPT], (partial,))
    pieces = lax.all_to_all(pieces.reshape(32, 1, 128), ("xl", "xh", FIRST), 0, 0, tiled=True)
    return call(final_kernel, jax.ShapeDtypeStruct((2, 4, 128), F32), [KEPT] * 2, (pieces.reshape(32, 128), fin))


def solution(mesh):
    axes = ("xl", "core", "xh", "z", "y")
    fine = Mesh(mesh.devices.reshape(2, 2, 2, 8, 8), axes)
    pix, scan = ("xl", "core"), ("xh", "z", "y")
    placed = (P(pix, scan, None), P(None, pix), P())
    return jax.shard_map(
        on_device, mesh=fine, in_specs=placed, out_specs=P(None, scan, pix), check_vma=False
    )
```

```python
import functools
import math

import jax
import jax.numpy as jnp
import numpy as np
from jax import lax
from jax.experimental import pallas as pl
from jax.experimental.pallas import tpu as pltpu
from jax.sharding import Mesh, PartitionSpec as P

STEP = 8
N = 512
BAND = 256
BOUND = 40.0 * STEP * STEP
VMEM = pl.BlockSpec(memory_space=pltpu.VMEM)
KEPT = pl.BlockSpec(memory_space=pltpu.VMEM)
SMALL = pl.BlockSpec(memory_space=pltpu.SMEM)
ANY = pl.BlockSpec(memory_space=pltpu.HBM)
BF = jnp.bfloat16
F32 = jnp.float32


def angles(k, n):
    return 2.0 * math.pi * np.mod(k * n, N) / N


def split(table):
    hi = table.astype(np.float32).astype(BF)
    lo = (table - hi.astype(np.float64)).astype(np.float32).astype(BF)
    return hi, lo


@functools.lru_cache(None)
def tables():
    jj, yy, c = np.meshgrid(np.arange(4), np.arange(8), np.arange(4), indexing="ij")
    ky = (8 * (4 * c + jj) + yy)[..., None]
    t = angles(ky, np.arange(N))
    row = np.stack([np.cos(t), -np.sin(t)], axis=3).reshape(256, N).astype(np.float32).astype(BF)
    kx = np.arange(BAND) - BAND // 2
    t = angles(np.arange(N)[:, None], kx[None, :])
    cos, sin = np.cos(t), np.sin(t)
    col = np.stack([np.concatenate([cos, -sin], 1), np.concatenate([sin, cos], 1)], axis=1)
    col = col.reshape(16, 64, 2 * BAND).astype(np.float32).astype(BF)
    place = (np.arange(16)[:, None, None] * 32 + np.arange(4)[:, None] + 4 * np.arange(8)).reshape(-1)
    inv = split(np.concatenate([cos.T[:, place], sin.T[:, place]], 1))
    yy, j = np.meshgrid(np.arange(8), np.arange(16), indexing="ij")
    ky = 8 * j + yy
    t = angles(ky[..., None], np.arange(N))
    fold = np.where(ky == 0, 1.0, 2.0)[..., None] / (N * N)
    real = np.where(ky == 0, 1.0, 0.0)[..., None] / (N * N)
    im = np.stack([np.sin(t) * fold, np.cos(t) * fold], axis=1)
    re = np.stack([np.cos(t) * real, -np.sin(t) * real], axis=1)
    fin = np.stack([re, im], axis=3).reshape(256, 2, 4, 128).transpose(2, 0, 1, 3).reshape(4, 256, 256)
    fin = np.stack(split(fin), axis=1)
    return row, col, np.stack(inv), fin


def swap_blocks(parts):
    lane = lax.broadcasted_iota(jnp.int32, parts[0].shape, 1) // 32
    out = []
    for m in range(4):
        acc = parts[0] if m == 0 else pltpu.roll(parts[0], (-32 * m) % 128, 1)
        for q in range(1, 4):
            shift = (32 * (q - m)) % 128
            moved = parts[q] if shift == 0 else pltpu.roll(parts[q], shift, 1)
            acc = jnp.where(lane == q, moved, acc)
        out.append(acc)
    return out


def row_kernel(table, data, out):
    held = data[...].reshape(128, N)
    spec = lax.dot_general(table[...], held, (((1,), (1,)), ((), ())), preferred_element_type=F32)
    parts = [spec[64 * q : 64 * q + 64] for q in range(4)]
    lane = lax.broadcasted_iota(jnp.int32, (64, 128), 1) % 4
    for r in range(4):
        moved = parts[r]
        for q in range(4):
            if q != r:
                moved = jnp.where(lane == q, pltpu.roll(parts[q], (q - r) % 128, 1), moved)
        out[:, r] = moved.reshape(8, 8, 128).astype(BF)


def weight_kernel(coefficients, coords, col, inv, fin, w_re, w_im, table, inv_out, fin_out, block, places, sems):
    here = lax.axis_index("xh") * 8 + lax.axis_index("z")
    group = lax.axis_index("xl") * 2 + lax.axis_index("core")
    copies = [
        pltpu.make_async_copy(col.at[here], block, sems.at[0]),
        pltpu.make_async_copy(inv, inv_out, sems.at[1]),
        pltpu.make_async_copy(fin.at[group], fin_out, sems.at[2]),
    ]
    for copy in copies:
        copy.start()

    a0 = coefficients[0] / (BOUND * math.pi)
    a1 = coefficients[1] / (BOUND * math.pi)
    a2 = coefficients[2] * 2.0 / (BOUND * math.pi)
    a3 = coefficients[3] / (BOUND * BOUND * math.pi)
    first = lax.axis_index("y").astype(F32)

    def chi(px, py, x2, y2, r2):
        return r2 * (a0 + a3 * r2) + (a1 * (x2 - y2) + a2 * (px * py))

    centre = coords[...].astype(F32) * float(STEP)
    source = lax.broadcasted_iota(jnp.int32, (32, 128), 0)
    target = lax.broadcasted_iota(jnp.int32, (32, 128), 1)
    centre = jnp.dot(centre, jnp.where(source == target // 4, 1.0, 0.0), preferred_element_type=F32)
    for n in range(2):
        places[n] = jnp.broadcast_to(centre[n : n + 1], (128, 128)).T
    wide, tall = places[0], places[1]
    places[2] = chi(wide, tall, wide * wide, tall * tall, wide * wide + tall * tall)
    step = first + 8.0 * (lax.broadcasted_iota(jnp.int32, (32, 128), 0) % 4).astype(F32)

    def one(n, carry):
        qy = step + 32.0 * (n // 4).astype(F32)
        here = pl.ds(pl.multiple_of(n % 4 * 32, 32), 32)
        kx, ky, own = places[0, here], places[1, here], places[2, here]
        rows = pl.ds(pl.multiple_of(n * 32, 32), 32)
        along = ky * qy
        for half in range(2):
            lanes = slice(128 * half, 128 * half + 128)
            qx = (lax.broadcasted_iota(jnp.int32, (32, 128), 1) + (128 * half - 128)).astype(F32)
            dot = kx * qx + along
            sign = jnp.where(dot > 0.0, 1.0, -1.0)
            px = kx - sign * qx
            py = ky - sign * qy
            x2 = px * px
            y2 = py * py
            near = x2 + y2
            far = near + 4.0 * jnp.abs(dot)
            phase = chi(px, py, x2, y2, near) - own
            turns = jnp.floor(phase + 0.5)
            f = phase - turns
            z = f * f
            sine = -0.00737043094571435 * z + 0.08214588661112823
            sine = sine * z - 0.5992645293207921
            sine = sine * z + 2.550164039877345
            sine = sine * z - 5.16771278004997
            sine = (sine * z + math.pi) * f
            cosine = 0.0019295743094039 * z - 0.02580689139001406
            cosine = cosine * z + 0.2353306303588935
            cosine = cosine * z - 1.3352627688545893
            cosine = cosine * z + 4.058712126416768
            cosine = cosine * z - 4.934802200544679
            cosine = cosine * z + 1.0
            pair = turns * 0.5
            flip = 1.0 - 4.0 * (pair - jnp.floor(pair))
            flip = jnp.where((near <= BOUND) & (far > BOUND), flip, 0.0)
            w_re[rows, lanes] = flip * sign * cosine
            w_im[rows, lanes] = flip * sine
        return carry

    lax.fori_loop(0, 16, one, 0)
    copies[0].wait()
    target = lax.broadcasted_iota(jnp.int32, (256, 64), 0)
    source = lax.broadcasted_iota(jnp.int32, (256, 64), 1)
    repeat = jnp.where(source == target // 8 * 2 + target % 2, 1.0, 0.0).astype(BF)
    table[...] = jnp.dot(repeat, block[...], preferred_element_type=F32).astype(BF)
    copies[1].wait()
    copies[2].wait()


def column_kernel(rows, table, w_re, w_im, inv, out, spec, total):
    held = rows[...].astype(F32).reshape(256, 128).T
    group = (lax.broadcasted_iota(jnp.int32, held.shape, 1) // 2) % 4
    stacked = jnp.concatenate([jnp.where(group == c, held, 0.0) for c in range(4)], axis=0).astype(BF)
    spec[...] = jnp.dot(stacked, table[...], preferred_element_type=F32)
    for c in range(4):
        part = slice(128 * c, 128 * c + 128)
        s_re, s_im = spec[part, :BAND], spec[part, BAND:]
        a, b = w_re[part, :], w_im[part, :]
        for n, z in enumerate((s_re * a - s_im * b, s_re * b + s_im * a)):
            pair = jnp.sum(z.reshape(16, 8, BAND), axis=0)
            total[16 * n + 4 * c : 16 * n + 4 * c + 4, :] = pair[:4] + pair[4:]
    whole = total[...]
    hi = whole.astype(BF)
    lo = (whole - hi.astype(F32)).astype(BF)
    both = jnp.dot(jnp.concatenate([hi, lo], axis=0), inv[0], preferred_element_type=F32)
    prod = both[:32] + both[32:] + jnp.dot(hi, inv[1], preferred_element_type=F32)
    c_re = prod[:16, :N] - prod[16:, N:]
    c_im = prod[:16, N:] + prod[16:, :N]
    quarters = [c_re[:8], c_re[8:], c_im[:8], c_im[8:]]
    for t in range(4):
        moved = swap_blocks([v[:, 128 * t : 128 * t + 128] for v in quarters])
        for m in range(4):
            for core in range(2):
                out[8 * core + 4 * (t % 2) + m, t // 2] = moved[m]


def regroup_kernel(parts, out):
    blocks = []
    for half in range(2):
        total = jnp.sum(parts[:, half], axis=0)
        blocks += [total if q == 0 else pltpu.roll(total, 128 - 32 * q, 1) for q in range(4)]
    turned = jnp.concatenate(blocks * 2, axis=0).T
    lane = lax.broadcasted_iota(jnp.int32, (8, 128), 1) // 32
    for half in range(2):
        acc = jnp.zeros((8, 128), F32)
        for r in range(4):
            piece = turned[8 * r : 8 * r + 8]
            shift = 32 * (r - half) % 128
            acc = jnp.where(lane == r, piece if shift == 0 else pltpu.roll(piece, shift, 1), acc)
        for g in range(2):
            out[16 * g + 8 * half : 16 * g + 8 * half + 8] = acc


def final_kernel(parts, table, out):
    total = parts[0:8]
    for n in range(1, 4):
        total = total + parts[8 * n : 8 * n + 8]
    turns = [total if s == 0 else pltpu.roll(total, 32 * s, 1) for s in range(4)]
    row = lax.broadcasted_iota(jnp.int32, (8, 128), 0) % 4
    lane = lax.broadcasted_iota(jnp.int32, (8, 128), 1) // 32
    rows = []
    for r in range(4):
        spread = jnp.zeros((8, 128), F32)
        for a in range(4):
            spread = jnp.where((row == a) & (lane == a), turns[(a - r) % 4], spread)
        low = jnp.sum(spread[:4], axis=0, keepdims=True)
        high = jnp.sum(spread[4:], axis=0, keepdims=True)
        rows.append(jnp.concatenate([low, high], axis=1))
    whole = jnp.concatenate(rows, axis=0)
    hi = whole.astype(BF)
    lo = (whole - hi.astype(F32)).astype(BF)
    both = jnp.dot(jnp.concatenate([hi, lo], axis=0), table[0], preferred_element_type=F32)
    obj = both[:4] + both[4:] + jnp.dot(hi, table[1], preferred_element_type=F32)
    out[0] = obj[:, :128]
    out[1] = obj[:, 128:]


def call(kernel, shapes, specs, operands, scratch=()):
    single = not isinstance(shapes, (list, tuple))
    count = 1 if single else len(shapes)
    spaces = [pltpu.VMEM if spec is KEPT else pltpu.SMEM if spec is SMALL else pltpu.HBM for spec in specs]
    held = [pltpu.with_memory_space_constraint(x, space) for x, space in zip(operands, spaces)]
    return pl.pallas_call(
        kernel,
        out_shape=shapes,
        in_specs=specs,
        out_specs=VMEM if single else [VMEM] * count,
        scratch_shapes=list(scratch),
        compiler_params=pltpu.CompilerParams(vmem_limit_bytes=16 * 2**20),
    )(*held)


def on_device(scan_data, pixel_coords, aberrations):
    row, col, inv, fin = (jnp.asarray(t) for t in tables())
    shape = pltpu.VMEM
    rows = call(row_kernel, shape((8, 4, 8, 128), BF), [VMEM] * 2, (row, scan_data))
    rows = lax.all_to_all(rows, "y", 0, 0, tiled=True)
    w_re, w_im, table, inv, fin = call(
        weight_kernel,
        [
            shape((512, BAND), F32),
            shape((512, BAND), F32),
            shape((256, N), BF),
            shape((2, 256, 2 * N), BF),
            shape((2, 256, 256), BF),
        ],
        [SMALL, KEPT, ANY, ANY, ANY],
        (aberrations, pixel_coords, col, inv, fin),
        scratch=[pltpu.VMEM((64, N), BF), pltpu.VMEM((3, 128, 128), F32), pltpu.SemaphoreType.DMA((3,))],
    )
    partial = call(
        column_kernel,
        shape((16, 2, 8, 128), F32),
        [KEPT] * 5,
        (rows, table, w_re, w_im, inv),
        scratch=[pltpu.VMEM((512, N), F32), pltpu.VMEM((32, BAND), F32)],
    )
    partial = lax.all_to_all(partial, ("core", "z"), 0, 0, tiled=True)
    pieces = call(regroup_kernel, shape((32, 128), F32), [KEPT], (partial,))
    pieces = lax.all_to_all(pieces.reshape(32, 1, 128), ("xl", "xh", "y"), 0, 0, tiled=True)
    return call(final_kernel, jax.ShapeDtypeStruct((2, 4, 128), F32), [KEPT] * 2, (pieces.reshape(32, 128), fin))


def solution(mesh):
    axes = ("xl", "core", "xh", "z", "y")
    fine = Mesh(mesh.devices.reshape(2, 2, 2, 8, 8), axes)
    pix, scan = ("xl", "core"), ("xh", "z", "y")
    placed = (P(pix, scan, None), P(None, pix), P())
    return jax.shard_map(
        on_device, mesh=fine, in_specs=placed, out_specs=P(None, scan, pix), check_vma=False
    )
```

```python
import functools
import math

import jax
import jax.numpy as jnp
import numpy as np
from jax import lax
from jax.experimental import pallas as pl
from jax.experimental.pallas import tpu as pltpu
from jax.sharding import Mesh, PartitionSpec as P

STEP = 8
N = 512
BAND = 256
BOUND = 40.0 * STEP * STEP
VMEM = pl.BlockSpec(memory_space=pltpu.VMEM)
KEPT = pl.BlockSpec(memory_space=pltpu.VMEM)
SMALL = pl.BlockSpec(memory_space=pltpu.SMEM)
ANY = pl.BlockSpec(memory_space=pltpu.HBM)
BF = jnp.bfloat16
F32 = jnp.float32


def angles(k, n):
    return 2.0 * math.pi * np.mod(k * n, N) / N


def split(table):
    hi = table.astype(np.float32).astype(BF)
    lo = (table - hi.astype(np.float64)).astype(np.float32).astype(BF)
    return hi, lo


@functools.lru_cache(None)
def tables():
    jj, yy, c = np.meshgrid(np.arange(4), np.arange(8), np.arange(4), indexing="ij")
    ky = (8 * (4 * c + jj) + yy)[..., None]
    t = angles(ky, np.arange(N // 2))
    row = np.stack([np.cos(t), -np.sin(t)], axis=3).reshape(256, N // 2).astype(np.float32).astype(BF)
    kx = np.arange(BAND) - BAND // 2
    t = angles(np.arange(N)[:, None], kx[None, :])
    cos, sin = np.cos(t), np.sin(t)
    col = np.stack([np.concatenate([cos, -sin], 1), np.concatenate([sin, cos], 1)], axis=1)
    col = col.reshape(16, 64, 2 * BAND).astype(np.float32).astype(BF)
    place = (np.arange(16)[:, None, None] * 32 + np.arange(4)[:, None] + 4 * np.arange(8)).reshape(-1)
    inv = split(np.concatenate([cos.T[:, place], sin.T[:, place]], 1))
    yy, j = np.meshgrid(np.arange(8), np.arange(16), indexing="ij")
    ky = 8 * j + yy
    t = angles(ky[..., None], np.arange(N))
    fold = np.where(ky == 0, 1.0, 2.0)[..., None] / (N * N)
    real = np.where(ky == 0, 1.0, 0.0)[..., None] / (N * N)
    im = np.stack([np.sin(t) * fold, np.cos(t) * fold], axis=1)
    re = np.stack([np.cos(t) * real, -np.sin(t) * real], axis=1)
    fin = np.stack([re, im], axis=3).reshape(256, 2, 4, 128).transpose(2, 0, 1, 3).reshape(4, 256, 256)
    fin = np.stack(split(fin), axis=1)
    return row, col, np.stack(inv), fin


def swap_blocks(parts):
    lane = lax.broadcasted_iota(jnp.int32, parts[0].shape, 1) // 32
    out = []
    for m in range(4):
        acc = parts[0] if m == 0 else pltpu.roll(parts[0], (-32 * m) % 128, 1)
        for q in range(1, 4):
            shift = (32 * (q - m)) % 128
            moved = parts[q] if shift == 0 else pltpu.roll(parts[q], shift, 1)
            acc = jnp.where(lane == q, moved, acc)
        out.append(acc)
    return out


def row_kernel(table, data, out):
    held = data[...].reshape(128, N)
    near, far = (
        lax.dot_general(table[...], half, (((1,), (1,)), ((), ())), preferred_element_type=F32)
        for half in (held[:, : N // 2], held[:, N // 2 :])
    )
    odd = lax.broadcasted_iota(jnp.int32, near.shape, 0) // 8 % 2 == 1
    spec = near + jnp.where(odd, -far, far)
    parts = [spec[64 * q : 64 * q + 64] for q in range(4)]
    lane = lax.broadcasted_iota(jnp.int32, (64, 128), 1) % 4
    for r in range(4):
        moved = parts[r]
        for q in range(4):
            if q != r:
                moved = jnp.where(lane == q, pltpu.roll(parts[q], (q - r) % 128, 1), moved)
        out[:, r] = moved.reshape(8, 8, 128).astype(BF)


def weight_kernel(coefficients, coords, col, inv, fin, w_re, w_im, table, inv_out, fin_out, block, places, sems):
    here = lax.axis_index("xh") * 8 + lax.axis_index("z")
    group = lax.axis_index("xl") * 2 + lax.axis_index("core")
    copies = [
        pltpu.make_async_copy(col.at[here], block, sems.at[0]),
        pltpu.make_async_copy(inv, inv_out, sems.at[1]),
        pltpu.make_async_copy(fin.at[group], fin_out, sems.at[2]),
    ]
    for copy in copies:
        copy.start()

    a0 = coefficients[0] / (BOUND * math.pi)
    a1 = coefficients[1] / (BOUND * math.pi)
    a2 = coefficients[2] * 2.0 / (BOUND * math.pi)
    a3 = coefficients[3] / (BOUND * BOUND * math.pi)
    first = lax.axis_index("y").astype(F32)

    def chi(px, py, x2, y2, r2):
        return r2 * (a0 + a3 * r2) + (a1 * (x2 - y2) + a2 * (px * py))

    centre = coords[...].astype(F32) * float(STEP)
    source = lax.broadcasted_iota(jnp.int32, (32, 128), 0)
    target = lax.broadcasted_iota(jnp.int32, (32, 128), 1)
    centre = jnp.dot(centre, jnp.where(source == target // 4, 1.0, 0.0), preferred_element_type=F32)
    for n in range(2):
        places[n] = jnp.broadcast_to(centre[n : n + 1], (128, 128)).T
    wide, tall = places[0], places[1]
    places[2] = chi(wide, tall, wide * wide, tall * tall, wide * wide + tall * tall)
    step = first + 8.0 * (lax.broadcasted_iota(jnp.int32, (32, 128), 0) % 4).astype(F32)

    def one(n, carry):
        qy = step + 32.0 * (n // 4).astype(F32)
        here = pl.ds(pl.multiple_of(n % 4 * 32, 32), 32)
        kx, ky, own = places[0, here], places[1, here], places[2, here]
        rows = pl.ds(pl.multiple_of(n * 32, 32), 32)
        along = ky * qy
        for half in range(2):
            lanes = slice(128 * half, 128 * half + 128)
            qx = (lax.broadcasted_iota(jnp.int32, (32, 128), 1) + (128 * half - 128)).astype(F32)
            dot = kx * qx + along
            sign = jnp.where(dot > 0.0, 1.0, -1.0)
            px = kx - sign * qx
            py = ky - sign * qy
            x2 = px * px
            y2 = py * py
            near = x2 + y2
            far = near + 4.0 * jnp.abs(dot)
            phase = chi(px, py, x2, y2, near) - own
            turns = jnp.floor(phase + 0.5)
            f = phase - turns
            z = f * f
            sine = -0.00737043094571435 * z + 0.08214588661112823
            sine = sine * z - 0.5992645293207921
            sine = sine * z + 2.550164039877345
            sine = sine * z - 5.16771278004997
            sine = (sine * z + math.pi) * f
            cosine = 0.0019295743094039 * z - 0.02580689139001406
            cosine = cosine * z + 0.2353306303588935
            cosine = cosine * z - 1.3352627688545893
            cosine = cosine * z + 4.058712126416768
            cosine = cosine * z - 4.934802200544679
            cosine = cosine * z + 1.0
            pair = turns * 0.5
            flip = 1.0 - 4.0 * (pair - jnp.floor(pair))
            flip = jnp.where((near <= BOUND) & (far > BOUND), flip, 0.0)
            w_re[rows, lanes] = flip * sign * cosine
            w_im[rows, lanes] = flip * sine
        return carry

    lax.fori_loop(0, 16, one, 0)
    copies[0].wait()
    target = lax.broadcasted_iota(jnp.int32, (256, 64), 0)
    source = lax.broadcasted_iota(jnp.int32, (256, 64), 1)
    repeat = jnp.where(source == target // 8 * 2 + target % 2, 1.0, 0.0).astype(BF)
    table[...] = jnp.dot(repeat, block[...], preferred_element_type=F32).astype(BF)
    copies[1].wait()
    copies[2].wait()


def column_kernel(rows, table, w_re, w_im, inv, out, spec, total):
    held = rows[...].astype(F32).reshape(256, 128).T
    group = (lax.broadcasted_iota(jnp.int32, held.shape, 1) // 2) % 4
    stacked = jnp.concatenate([jnp.where(group == c, held, 0.0) for c in range(4)], axis=0).astype(BF)
    spec[...] = jnp.dot(stacked, table[...], preferred_element_type=F32)
    for c in range(4):
        part = slice(128 * c, 128 * c + 128)
        s_re, s_im = spec[part, :BAND], spec[part, BAND:]
        a, b = w_re[part, :], w_im[part, :]
        for n, z in enumerate((s_re * a - s_im * b, s_re * b + s_im * a)):
            pair = jnp.sum(z.reshape(16, 8, BAND), axis=0)
            total[16 * n + 4 * c : 16 * n + 4 * c + 4, :] = pair[:4] + pair[4:]
    whole = total[...]
    hi = whole.astype(BF)
    lo = (whole - hi.astype(F32)).astype(BF)
    both = jnp.dot(jnp.concatenate([hi, lo], axis=0), inv[0], preferred_element_type=F32)
    prod = both[:32] + both[32:] + jnp.dot(hi, inv[1], preferred_element_type=F32)
    c_re = prod[:16, :N] - prod[16:, N:]
    c_im = prod[:16, N:] + prod[16:, :N]
    quarters = [c_re[:8], c_re[8:], c_im[:8], c_im[8:]]
    for t in range(4):
        moved = swap_blocks([v[:, 128 * t : 128 * t + 128] for v in quarters])
        for m in range(4):
            for core in range(2):
                out[8 * core + 4 * (t % 2) + m, t // 2] = moved[m]


def regroup_kernel(parts, out):
    blocks = []
    for half in range(2):
        total = jnp.sum(parts[:, half], axis=0)
        blocks += [total if q == 0 else pltpu.roll(total, 128 - 32 * q, 1) for q in range(4)]
    turned = jnp.concatenate(blocks * 2, axis=0).T
    lane = lax.broadcasted_iota(jnp.int32, (8, 128), 1) // 32
    for half in range(2):
        acc = jnp.zeros((8, 128), F32)
        for r in range(4):
            piece = turned[8 * r : 8 * r + 8]
            shift = 32 * (r - half) % 128
            acc = jnp.where(lane == r, piece if shift == 0 else pltpu.roll(piece, shift, 1), acc)
        for g in range(2):
            out[16 * g + 8 * half : 16 * g + 8 * half + 8] = acc


def final_kernel(parts, table, out):
    total = parts[0:8]
    for n in range(1, 4):
        total = total + parts[8 * n : 8 * n + 8]
    turns = [total if s == 0 else pltpu.roll(total, 32 * s, 1) for s in range(4)]
    row = lax.broadcasted_iota(jnp.int32, (8, 128), 0) % 4
    lane = lax.broadcasted_iota(jnp.int32, (8, 128), 1) // 32
    rows = []
    for r in range(4):
        spread = jnp.zeros((8, 128), F32)
        for a in range(4):
            spread = jnp.where((row == a) & (lane == a), turns[(a - r) % 4], spread)
        low = jnp.sum(spread[:4], axis=0, keepdims=True)
        high = jnp.sum(spread[4:], axis=0, keepdims=True)
        rows.append(jnp.concatenate([low, high], axis=1))
    whole = jnp.concatenate(rows, axis=0)
    hi = whole.astype(BF)
    lo = (whole - hi.astype(F32)).astype(BF)
    both = jnp.dot(jnp.concatenate([hi, lo], axis=0), table[0], preferred_element_type=F32)
    obj = both[:4] + both[4:] + jnp.dot(hi, table[1], preferred_element_type=F32)
    out[0] = obj[:, :128]
    out[1] = obj[:, 128:]


def call(kernel, shapes, specs, operands, scratch=()):
    single = not isinstance(shapes, (list, tuple))
    count = 1 if single else len(shapes)
    spaces = [pltpu.VMEM if spec is KEPT else pltpu.SMEM if spec is SMALL else pltpu.HBM for spec in specs]
    held = [pltpu.with_memory_space_constraint(x, space) for x, space in zip(operands, spaces)]
    return pl.pallas_call(
        kernel,
        out_shape=shapes,
        in_specs=specs,
        out_specs=VMEM if single else [VMEM] * count,
        scratch_shapes=list(scratch),
        compiler_params=pltpu.CompilerParams(vmem_limit_bytes=16 * 2**20),
    )(*held)


def on_device(scan_data, pixel_coords, aberrations):
    row, col, inv, fin = (jnp.asarray(t) for t in tables())
    shape = pltpu.VMEM
    rows = call(row_kernel, shape((8, 4, 8, 128), BF), [VMEM] * 2, (row, scan_data))
    rows = lax.all_to_all(rows, "y", 0, 0, tiled=True)
    w_re, w_im, table, inv, fin = call(
        weight_kernel,
        [
            shape((512, BAND), F32),
            shape((512, BAND), F32),
            shape((256, N), BF),
            shape((2, 256, 2 * N), BF),
            shape((2, 256, 256), BF),
        ],
        [SMALL, KEPT, ANY, ANY, ANY],
        (aberrations, pixel_coords, col, inv, fin),
        scratch=[pltpu.VMEM((64, N), BF), pltpu.VMEM((3, 128, 128), F32), pltpu.SemaphoreType.DMA((3,))],
    )
    partial = call(
        column_kernel,
        shape((16, 2, 8, 128), F32),
        [KEPT] * 5,
        (rows, table, w_re, w_im, inv),
        scratch=[pltpu.VMEM((512, N), F32), pltpu.VMEM((32, BAND), F32)],
    )
    partial = lax.all_to_all(partial, ("core", "z"), 0, 0, tiled=True)
    pieces = call(regroup_kernel, shape((32, 128), F32), [KEPT], (partial,))
    pieces = lax.all_to_all(pieces.reshape(32, 1, 128), ("xl", "xh", "y"), 0, 0, tiled=True)
    return call(final_kernel, jax.ShapeDtypeStruct((2, 4, 128), F32), [KEPT] * 2, (pieces.reshape(32, 128), fin))


def solution(mesh):
    axes = ("xl", "core", "xh", "z", "y")
    fine = Mesh(mesh.devices.reshape(2, 2, 2, 8, 8), axes)
    pix, scan = ("xl", "core"), ("xh", "z", "y")
    placed = (P(pix, scan, None), P(None, pix), P())
    return jax.shard_map(
        on_device, mesh=fine, in_specs=placed, out_specs=P(None, scan, pix), check_vma=False
    )
```

```python
import functools
import math

import jax
import jax.numpy as jnp
import numpy as np
from jax import lax
from jax.experimental import pallas as pl
from jax.experimental.pallas import tpu as pltpu
from jax.sharding import Mesh, PartitionSpec as P

STEP = 8
N = 512
BAND = 256
BOUND = 40.0 * STEP * STEP
VMEM = pl.BlockSpec(memory_space=pltpu.VMEM)
KEPT = pl.BlockSpec(memory_space=pltpu.VMEM)
SMALL = pl.BlockSpec(memory_space=pltpu.SMEM)
ANY = pl.BlockSpec(memory_space=pltpu.HBM)
BF = jnp.bfloat16
F32 = jnp.float32


def angles(k, n):
    return 2.0 * math.pi * np.mod(k * n, N) / N


def split(table):
    hi = table.astype(np.float32).astype(BF)
    lo = (table - hi.astype(np.float64)).astype(np.float32).astype(BF)
    return hi, lo


@functools.lru_cache(None)
def tables():
    jj, yy, c = np.meshgrid(np.arange(4), np.arange(8), np.arange(4), indexing="ij")
    ky = (8 * (4 * c + jj) + yy)[..., None]
    t = angles(ky, np.arange(N // 2))
    row = np.stack([np.cos(t), -np.sin(t)], axis=3).reshape(256, N // 2).astype(np.float32).astype(BF)
    kx = np.arange(BAND) - BAND // 2
    t = angles(np.arange(N)[:, None], kx[None, :])
    cos, sin = np.cos(t), np.sin(t)
    col = np.stack([np.concatenate([cos, -sin], 1), np.concatenate([sin, cos], 1)], axis=1)
    col = col.reshape(16, 64, 2 * BAND).astype(np.float32).astype(BF)
    place = (np.arange(16)[:, None, None] * 32 + np.arange(4)[:, None] + 4 * np.arange(8)).reshape(-1)
    place = place[: N // 2]
    inv = split(np.concatenate([cos.T[:, place], sin.T[:, place]], 1))
    yy, j = np.meshgrid(np.arange(8), np.arange(16), indexing="ij")
    ky = 8 * j + yy
    t = angles(ky[..., None], np.arange(N))
    fold = np.where(ky == 0, 1.0, 2.0)[..., None] / (N * N)
    real = np.where(ky == 0, 1.0, 0.0)[..., None] / (N * N)
    im = np.stack([np.sin(t) * fold, np.cos(t) * fold], axis=1)
    re = np.stack([np.cos(t) * real, -np.sin(t) * real], axis=1)
    fin = np.stack([re, im], axis=3).reshape(256, 2, 4, 128).transpose(2, 0, 1, 3).reshape(4, 256, 256)
    fin = np.stack(split(fin), axis=1)
    return row, col, np.stack(inv), fin


def swap_blocks(parts):
    lane = lax.broadcasted_iota(jnp.int32, parts[0].shape, 1) // 32
    out = []
    for m in range(4):
        acc = parts[0] if m == 0 else pltpu.roll(parts[0], (-32 * m) % 128, 1)
        for q in range(1, 4):
            shift = (32 * (q - m)) % 128
            moved = parts[q] if shift == 0 else pltpu.roll(parts[q], shift, 1)
            acc = jnp.where(lane == q, moved, acc)
        out.append(acc)
    return out


def row_kernel(table, data, out):
    held = data[...].reshape(128, N)
    near, far = (
        lax.dot_general(table[...], half, (((1,), (1,)), ((), ())), preferred_element_type=F32)
        for half in (held[:, : N // 2], held[:, N // 2 :])
    )
    odd = lax.broadcasted_iota(jnp.int32, near.shape, 0) // 8 % 2 == 1
    spec = near + jnp.where(odd, -far, far)
    parts = [spec[64 * q : 64 * q + 64] for q in range(4)]
    lane = lax.broadcasted_iota(jnp.int32, (64, 128), 1) % 4
    for r in range(4):
        moved = parts[r]
        for q in range(4):
            if q != r:
                moved = jnp.where(lane == q, pltpu.roll(parts[q], (q - r) % 128, 1), moved)
        out[:, r] = moved.reshape(8, 8, 128).astype(BF)


def weight_kernel(coefficients, coords, col, inv, fin, w_re, w_im, table, inv_out, fin_out, block, places, sems):
    here = lax.axis_index("xh") * 8 + lax.axis_index("z")
    group = lax.axis_index("xl") * 2 + lax.axis_index("core")
    copies = [
        pltpu.make_async_copy(col.at[here], block, sems.at[0]),
        pltpu.make_async_copy(inv, inv_out, sems.at[1]),
        pltpu.make_async_copy(fin.at[group], fin_out, sems.at[2]),
    ]
    for copy in copies:
        copy.start()

    a0 = coefficients[0] / (BOUND * math.pi)
    a1 = coefficients[1] / (BOUND * math.pi)
    a2 = coefficients[2] * 2.0 / (BOUND * math.pi)
    a3 = coefficients[3] / (BOUND * BOUND * math.pi)
    first = lax.axis_index("y").astype(F32)

    def chi(px, py, x2, y2, r2):
        return r2 * (a0 + a3 * r2) + (a1 * (x2 - y2) + a2 * (px * py))

    centre = coords[...].astype(F32) * float(STEP)
    source = lax.broadcasted_iota(jnp.int32, (32, 128), 0)
    target = lax.broadcasted_iota(jnp.int32, (32, 128), 1)
    centre = jnp.dot(centre, jnp.where(source == target // 4, 1.0, 0.0), preferred_element_type=F32)
    for n in range(2):
        places[n] = jnp.broadcast_to(centre[n : n + 1], (128, 128)).T
    wide, tall = places[0], places[1]
    places[2] = chi(wide, tall, wide * wide, tall * tall, wide * wide + tall * tall)
    step = first + 8.0 * (lax.broadcasted_iota(jnp.int32, (32, 128), 0) % 4).astype(F32)

    def one(n, carry):
        qy = step + 32.0 * (n // 4).astype(F32)
        here = pl.ds(pl.multiple_of(n % 4 * 32, 32), 32)
        kx, ky, own = places[0, here], places[1, here], places[2, here]
        rows = pl.ds(pl.multiple_of(n * 32, 32), 32)
        along = ky * qy
        for half in range(2):
            lanes = slice(128 * half, 128 * half + 128)
            qx = (lax.broadcasted_iota(jnp.int32, (32, 128), 1) + (128 * half - 128)).astype(F32)
            dot = kx * qx + along
            sign = jnp.where(dot > 0.0, 1.0, -1.0)
            px = kx - sign * qx
            py = ky - sign * qy
            x2 = px * px
            y2 = py * py
            near = x2 + y2
            far = near + 4.0 * jnp.abs(dot)
            phase = chi(px, py, x2, y2, near) - own
            turns = jnp.floor(phase + 0.5)
            f = phase - turns
            z = f * f
            sine = -0.00737043094571435 * z + 0.08214588661112823
            sine = sine * z - 0.5992645293207921
            sine = sine * z + 2.550164039877345
            sine = sine * z - 5.16771278004997
            sine = (sine * z + math.pi) * f
            cosine = 0.0019295743094039 * z - 0.02580689139001406
            cosine = cosine * z + 0.2353306303588935
            cosine = cosine * z - 1.3352627688545893
            cosine = cosine * z + 4.058712126416768
            cosine = cosine * z - 4.934802200544679
            cosine = cosine * z + 1.0
            pair = turns * 0.5
            flip = 1.0 - 4.0 * (pair - jnp.floor(pair))
            flip = jnp.where((near <= BOUND) & (far > BOUND), flip, 0.0)
            w_re[rows, lanes] = flip * sign * cosine
            w_im[rows, lanes] = flip * sine
        return carry

    lax.fori_loop(0, 16, one, 0)
    copies[0].wait()
    target = lax.broadcasted_iota(jnp.int32, (256, 64), 0)
    source = lax.broadcasted_iota(jnp.int32, (256, 64), 1)
    repeat = jnp.where(source == target // 8 * 2 + target % 2, 1.0, 0.0).astype(BF)
    table[...] = jnp.dot(repeat, block[...], preferred_element_type=F32).astype(BF)
    copies[1].wait()
    copies[2].wait()


def column_kernel(rows, table, w_re, w_im, inv, out, spec, total):
    held = rows[...].astype(F32).reshape(256, 128).T
    group = (lax.broadcasted_iota(jnp.int32, held.shape, 1) // 2) % 4
    stacked = jnp.concatenate([jnp.where(group == c, held, 0.0) for c in range(4)], axis=0).astype(BF)
    spec[...] = jnp.dot(stacked, table[...], preferred_element_type=F32)
    for c in range(4):
        part = slice(128 * c, 128 * c + 128)
        s_re, s_im = spec[part, :BAND], spec[part, BAND:]
        a, b = w_re[part, :], w_im[part, :]
        for n, z in enumerate((s_re * a - s_im * b, s_re * b + s_im * a)):
            pair = jnp.sum(z.reshape(16, 8, BAND), axis=0)
            total[16 * n + 4 * c : 16 * n + 4 * c + 4, :] = pair[:4] + pair[4:]
    whole = total[...]
    even = lax.broadcasted_iota(jnp.int32, whole.shape, 1) % 2 == 0
    whole = jnp.concatenate([jnp.where(even, whole, 0.0), jnp.where(even, 0.0, whole)], axis=0)
    hi = whole.astype(BF)
    lo = (whole - hi.astype(F32)).astype(BF)
    both = jnp.dot(jnp.concatenate([hi, lo], axis=0), inv[0], preferred_element_type=F32)
    prod = both[:64] + both[64:] + jnp.dot(hi, inv[1], preferred_element_type=F32)
    for half, p in enumerate((prod[:32] + prod[32:], prod[:32] - prod[32:])):
        c_re = p[:16, : N // 2] - p[16:, N // 2 :]
        c_im = p[:16, N // 2 :] + p[16:, : N // 2]
        quarters = [c_re[:8], c_re[8:], c_im[:8], c_im[8:]]
        for t in range(2):
            moved = swap_blocks([v[:, 128 * t : 128 * t + 128] for v in quarters])
            for m in range(4):
                for core in range(2):
                    out[8 * core + 4 * t + m, half] = moved[m]


def regroup_kernel(parts, out):
    blocks = []
    for half in range(2):
        total = jnp.sum(parts[:, half], axis=0)
        blocks += [total if q == 0 else pltpu.roll(total, 128 - 32 * q, 1) for q in range(4)]
    turned = jnp.concatenate(blocks * 2, axis=0).T
    lane = lax.broadcasted_iota(jnp.int32, (8, 128), 1) // 32
    for half in range(2):
        acc = jnp.zeros((8, 128), F32)
        for r in range(4):
            piece = turned[8 * r : 8 * r + 8]
            shift = 32 * (r - half) % 128
            acc = jnp.where(lane == r, piece if shift == 0 else pltpu.roll(piece, shift, 1), acc)
        for g in range(2):
            out[16 * g + 8 * half : 16 * g + 8 * half + 8] = acc


def final_kernel(parts, table, out):
    total = parts[0:8]
    for n in range(1, 4):
        total = total + parts[8 * n : 8 * n + 8]
    turns = [total if s == 0 else pltpu.roll(total, 32 * s, 1) for s in range(4)]
    row = lax.broadcasted_iota(jnp.int32, (8, 128), 0) % 4
    lane = lax.broadcasted_iota(jnp.int32, (8, 128), 1) // 32
    rows = []
    for r in range(4):
        spread = jnp.zeros((8, 128), F32)
        for a in range(4):
            spread = jnp.where((row == a) & (lane == a), turns[(a - r) % 4], spread)
        low = jnp.sum(spread[:4], axis=0, keepdims=True)
        high = jnp.sum(spread[4:], axis=0, keepdims=True)
        rows.append(jnp.concatenate([low, high], axis=1))
    whole = jnp.concatenate(rows, axis=0)
    hi = whole.astype(BF)
    lo = (whole - hi.astype(F32)).astype(BF)
    both = jnp.dot(jnp.concatenate([hi, lo], axis=0), table[0], preferred_element_type=F32)
    obj = both[:4] + both[4:] + jnp.dot(hi, table[1], preferred_element_type=F32)
    out[0] = obj[:, :128]
    out[1] = obj[:, 128:]


def call(kernel, shapes, specs, operands, scratch=()):
    single = not isinstance(shapes, (list, tuple))
    count = 1 if single else len(shapes)
    spaces = [pltpu.VMEM if spec is KEPT else pltpu.SMEM if spec is SMALL else pltpu.HBM for spec in specs]
    held = [pltpu.with_memory_space_constraint(x, space) for x, space in zip(operands, spaces)]
    return pl.pallas_call(
        kernel,
        out_shape=shapes,
        in_specs=specs,
        out_specs=VMEM if single else [VMEM] * count,
        scratch_shapes=list(scratch),
        compiler_params=pltpu.CompilerParams(vmem_limit_bytes=16 * 2**20),
    )(*held)


def on_device(scan_data, pixel_coords, aberrations):
    row, col, inv, fin = (jnp.asarray(t) for t in tables())
    shape = pltpu.VMEM
    rows = call(row_kernel, shape((8, 4, 8, 128), BF), [VMEM] * 2, (row, scan_data))
    rows = lax.all_to_all(rows, "y", 0, 0, tiled=True)
    w_re, w_im, table, inv, fin = call(
        weight_kernel,
        [
            shape((512, BAND), F32),
            shape((512, BAND), F32),
            shape((256, N), BF),
            shape((2, 256, N), BF),
            shape((2, 256, 256), BF),
        ],
        [SMALL, KEPT, ANY, ANY, ANY],
        (aberrations, pixel_coords, col, inv, fin),
        scratch=[pltpu.VMEM((64, N), BF), pltpu.VMEM((3, 128, 128), F32), pltpu.SemaphoreType.DMA((3,))],
    )
    partial = call(
        column_kernel,
        shape((16, 2, 8, 128), F32),
        [KEPT] * 5,
        (rows, table, w_re, w_im, inv),
        scratch=[pltpu.VMEM((512, N), F32), pltpu.VMEM((32, BAND), F32)],
    )
    partial = lax.all_to_all(partial, ("core", "z"), 0, 0, tiled=True)
    pieces = call(regroup_kernel, shape((32, 128), F32), [KEPT], (partial,))
    pieces = lax.all_to_all(pieces.reshape(32, 1, 128), ("xl", "xh", "y"), 0, 0, tiled=True)
    return call(final_kernel, jax.ShapeDtypeStruct((2, 4, 128), F32), [KEPT] * 2, (pieces.reshape(32, 128), fin))


def solution(mesh):
    axes = ("xl", "core", "xh", "z", "y")
    fine = Mesh(mesh.devices.reshape(2, 2, 2, 8, 8), axes)
    pix, scan = ("xl", "core"), ("xh", "z", "y")
    placed = (P(pix, scan, None), P(None, pix), P())
    return jax.shard_map(
        on_device, mesh=fine, in_specs=placed, out_specs=P(None, scan, pix), check_vma=False
    )
```
